32 devices in a mesh: lat: 8 (over y, x, core), lon: 4 (over z).
Axes of the slice: x: 2, y: 2, z: 4, core: 2. Of those that a mesh axis runs over, the one named last changes fastest.
Arguments:
- right_side: float32 [256, 4096], P('lat', 'lon'), may hold values from -6 to 6
- coefficients: float32 [4, 256, 4096], P(None, 'lat', 'lon'), may hold values from 0.2 to 1.2
- extra: float32 [256, 4096], P('lat', 'lon'), may hold values from 0.05 to 1
- land_mask: int32 [256, 4096], P('lat', 'lon'), may hold values 0 or 1
Outputs:
- solution_field: float32 [256, 4096], P('lat', 'lon')
- residual: float32 [256, 4096], P('lat', 'lon')
- norms: float32 [3], replicated
The draws below stay inside these ranges and needn't reach their ends.
All inputs are finite; a program needn't handle non-finite values. No bound on the sum of `land_mask` on one device may be relied on, other than what follows from the above.
Results may differ from the reference program's by a relative error of at most 0.00028.
Values sent between devices are 32-bit elements; how exact they have to be, the bound alone decides.
A program may use at most 64 MiB of HBM per device.

```python
import math
import jax
import jax.numpy as jnp

DEG = 4
ITERS = 3
NY = 256
NX = 4096


def touch_ends(array, stream_key, least, largest):
    extent = array.shape
    place = [jax.random.randint(jax.random.fold_in(stream_key, axis), (), 0, extent[axis]) for axis in range(len(extent))]
    array = array.at[tuple(place)].set(least)
    longest = extent.index(max(extent))
    place[longest] = (place[longest] + 1) % extent[longest]
    return array.at[tuple(place)].set(largest)


def steps_of(own_key, dims, cuts, least, top_value):
    factor_of, own = 1.0, jax.random.fold_in(own_key, 6)
    for dim, parts in cuts:
        draws = jnp.exp(jax.random.uniform(jax.random.fold_in(own, dim), (parts,), jnp.float32, least / len(cuts), top_value / len(cuts)))
        factor_of = factor_of * jnp.repeat(draws, dims[dim] // parts).reshape([-1 if axis == dim else 1 for axis in range(len(dims))])
    return factor_of


def noise(own_key, dims, deviation, reach, split=(), kind=jnp.bfloat16):
    array = deviation * jax.random.normal(own_key, dims, jnp.float32)
    if split:
        array = array * steps_of(own_key, dims, split, -0.22, 0.18)
    return jnp.clip(array, -reach, reach).astype(kind)


def setup_inputs(seed: int = 0) -> dict:
    splits = jax.random.split(jax.random.key(seed), 5)
    right_side = noise(splits[0], (NY, NX), 1.0, 6.0, ((0, 8), (1, 4)), jnp.float32)
    coefficients = jnp.clip(0.2 + 1 * jax.random.uniform(splits[1], (4, NY, NX), jnp.float32) ** steps_of(splits[1], (4, NY, NX), ((1, 8), (2, 4)), -0.2, 0.2), 0.2, 1.2)
    extra = jnp.clip(jnp.exp(math.log(1.0) - 2.9957323 * jax.random.uniform(splits[2], (NY, NX), jnp.float32) ** steps_of(splits[2], (NY, NX), ((0, 8), (1, 4)), -0.2, 0.2)), 0.05, 1.0)
    land_mask = touch_ends((jax.random.randint(splits[3], (NY, NX), 0, 5) < 4).astype(jnp.int32), jax.random.fold_in(splits[3], 1), 0, 1)
    return {"right_side": right_side, "coefficients": coefficients, "extra": extra, "land_mask": land_mask}


LOW_EIG = 0.25
HIGH_EIG = 20.5


def east(a):
    return jnp.roll(a, -1, axis=1)


def west(a):
    return jnp.roll(a, 1, axis=1)


def north(a):
    return jnp.roll(a, -1, axis=0)


def south(a):
    return jnp.roll(a, 1, axis=0)


def operate(v, diag, le, ln, lne, lnw):
    out = diag * v - le * east(v) - west(le) * west(v)
    out = out - ln * north(v) - south(ln) * south(v)
    out = out - lne * north(east(v)) - south(west(lne)) * south(west(v))
    out = out - lnw * north(west(v)) - south(east(lnw)) * south(east(v))
    return out


def chebyshev(r, mat):
    theta = (HIGH_EIG + LOW_EIG) / 2.0
    delta = (HIGH_EIG - LOW_EIG) / 2.0
    sigma = theta / delta
    rho = 1.0 / sigma
    step = r / theta
    z = step
    for level in range(DEG - 1):
        q = r - mat(z)
        rho_new = 1.0 / (2.0 * sigma - rho)
        step = (rho_new * rho) * step + (2.0 * rho_new / delta) * q
        z = z + step
        rho = rho_new
    return z


def reference(right_side, coefficients, extra, land_mask):
    m = land_mask.astype(jnp.float32)
    rows = jnp.arange(NY, dtype=jnp.int32)
    keep = (rows != NY - 1).astype(jnp.float32)[:, None]
    le = coefficients[0] * m * east(m)
    ln = coefficients[1] * m * north(m) * keep
    lne = coefficients[2] * m * north(east(m)) * keep
    lnw = coefficients[3] * m * north(west(m)) * keep
    diag = extra + le + west(le) + ln + south(ln) + lne + south(west(lne)) + lnw + south(east(lnw))

    def mat(v):
        return operate(v, diag, le, ln, lne, lnw)

    r = m * right_side
    x = jnp.zeros_like(r)
    u = chebyshev(r, mat)
    w = mat(u)
    gamma = jnp.sum(r * u)
    dlt = jnp.sum(w * u)
    norms = [jnp.sum(r * r)]
    alpha = gamma / dlt
    p = u
    s = w
    beta = jnp.float32(0.0)
    for k in range(ITERS):
        if k > 0:
            p = u + beta * p
            s = w + beta * s
        x = x + alpha * p
        r = r - alpha * s
        if k < ITERS - 1:
            u = chebyshev(r, mat)
            w = mat(u)
            gamma_new = jnp.sum(r * u)
            dlt = jnp.sum(w * u)
            norms.append(jnp.sum(r * r))
            beta = gamma_new / gamma
            alpha = gamma_new / (dlt - beta * gamma_new / alpha)
            gamma = gamma_new
    return x, r, jnp.stack(norms).astype(jnp.float32)
```

```python
import functools

import jax
import jax.numpy as jnp
from jax import lax
from jax.experimental import pallas as pl
from jax.experimental.pallas import tpu as pltpu
from jax.sharding import PartitionSpec as P

DEG = 4
ITERS = 3
LOW_EIG = 0.25
HIGH_EIG = 20.5
SHIFT = 0.8
LANES = 128
HALO = 16
VMEM_GRANT = 24 * 1024 * 1024
STRIP = 16
FIELDS = 7
PAIRS = (FIELDS + 1) // 2
MESH = pl.DeviceIdType.MESH
DIRS = [(a, b) for a in (-1, 0, 1) for b in (-1, 0, 1) if (a, b) != (0, 0)]


def level_factors():
    theta = (HIGH_EIG + LOW_EIG) / 2.0
    delta = (HIGH_EIG - LOW_EIG) / 2.0
    sigma = theta / delta
    rho = 1.0 / sigma
    out = []
    for _ in range(DEG - 1):
        rho_new = 1.0 / (2.0 * sigma - rho)
        out.append((rho_new * rho, 2.0 * rho_new / delta))
        rho = rho_new
    return theta, out


def scalars(h, g):
    c = SHIFT
    ht = [h[k + 1] + c * h[k] for k in range(len(h) - 1)]

    def form(a, t):
        total = None
        for k in range(2 * len(a) - 1):
            pairs = None
            for i in range(len(a)):
                j = k - i
                if 0 <= j < len(a) and i <= j:
                    term = a[i] * a[j]
                    if i != j:
                        term = term + term
                    pairs = term if pairs is None else pairs + term
            pairs = pairs * t[k]
            total = pairs if total is None else total + pairs
        return total

    one = jnp.ones_like(h[0])
    zero = jnp.zeros_like(h[0])
    a = [one]
    b = [one]
    gamma = h[0]
    norms = [g[0]]
    alpha = gamma / ht[0]
    x = [zero] * ITERS
    beta = zero
    for k in range(ITERS):
        if k > 0:
            b = [a[i] + (beta * b[i] if i < len(b) else 0.0) for i in range(len(a))]
        for i in range(len(b)):
            x[i] = x[i] + alpha * b[i]
        tb = [
            (b[i - 1] if i > 0 else zero) + (c * b[i] if i < len(b) else zero)
            for i in range(len(b) + 1)
        ]
        a = [(a[i] if i < len(a) else zero) - alpha * tb[i] for i in range(len(tb))]
        if k < ITERS - 1:
            gamma_new = form(a, h)
            dlt = form(a, ht)
            norms.append(form(a, g))
            beta = gamma_new / gamma
            alpha = gamma_new / (dlt - beta * gamma_new / alpha)
            gamma = gamma_new
    return x, a, norms


def kernel(
    nlat, nlon, rhs_in, coef_in, extra_in, mask_in, V, U, T_out,
    B, C, E, M, K, VC, UC, S, Z, SP, RP, SR, RR, G, GL, GZ, T2,
    loc_sem, snd, rcv, lat_s, lat_r, lon_s, lon_r,
):
    rows, cols = rhs_in.shape
    R = rows + 2 * HALO
    W = cols + 2 * LANES
    NC = W // LANES
    ilat = lax.axis_index("lat")
    ilon = lax.axis_index("lon")

    def cs_of(j):
        return slice(j * LANES, (j + 1) * LANES)

    mid = (pl.ds(HALO, rows), pl.ds(LANES, cols))
    local = [
        pltpu.make_async_copy(coef_in, C.at[:, mid[0], mid[1]], loc_sem.at[0]),
        pltpu.make_async_copy(mask_in, M.at[mid[0], mid[1]], loc_sem.at[1]),
        pltpu.make_async_copy(extra_in, E.at[mid[0], mid[1]], loc_sem.at[2]),
        pltpu.make_async_copy(rhs_in, B.at[mid[0], mid[1]], loc_sem.at[3]),
    ]
    for cp in local:
        cp.start()

    def lat_at(d):
        return lax.rem(ilat + d + nlat, nlat)

    def lon_at(d):
        return lax.rem(ilon + d + nlon, nlon)

    barrier = pltpu.get_barrier_semaphore()
    count = 0
    for d in range(1, nlat):
        pl.semaphore_signal(barrier, inc=1, device_id={"lat": lat_at(d)}, device_id_type=MESH)
        count += 1
    for d in range(1, nlon):
        pl.semaphore_signal(barrier, inc=1, device_id={"lon": lon_at(d)}, device_id_type=MESH)
        count += 1
    for a, b in DIRS:
        if a and b:
            pl.semaphore_signal(
                barrier, inc=1, device_id={"lat": lat_at(a), "lon": lon_at(b)}, device_id_type=MESH
            )
            count += 1

    def field(f, rws, cls):
        if f < 4:
            return C[f, rws, cls]
        if f == 4:
            return E[rws, cls]
        if f == 5:
            return B[rws, cls]
        return M[rws, cls].astype(jnp.float32)

    def put(f, rws, cls, value):
        if f < 4:
            C[f, rws, cls] = value
        elif f == 4:
            E[rws, cls] = value
        elif f == 5:
            B[rws, cls] = value
        else:
            M[rws, cls] = value.astype(jnp.int32)

    pl.semaphore_wait(barrier, count)

    sends = []

    def send(src, dst, a, b):
        i = len(sends)
        where = {}
        if a:
            where["lat"] = lat_at(a)
        if b:
            where["lon"] = lon_at(b)
        cp = pltpu.make_async_remote_copy(
            src_ref=src, dst_ref=dst, send_sem=snd.at[i], recv_sem=rcv.at[i],
            device_id=where, device_id_type=MESH,
        )
        cp.start()
        sends.append(cp)

    wide = pl.ds(LANES, cols)
    spans = {
        -1: (pl.ds(HALO, 8), pl.ds(HALO + rows, 8)),
        1: (pl.ds(HALO + rows - 8, 8), pl.ds(HALO - 8, 8)),
    }
    for ref, cp in zip((C, M, E, B), local):
        cp.wait()
        for a, (src, dst) in spans.items():
            if ref is C:
                send(C.at[:, src, wide], C.at[:, dst, wide], a, 0)
            else:
                send(ref.at[src, wide], ref.at[dst, wide], a, 0)

    own_rows = slice(HALO, HALO + rows)
    slot = lax.broadcasted_iota(jnp.int32, (rows, LANES), 1) // STRIP
    for side, chunk in ((0, 1), (1, NC - 2)):
        strip = jnp.zeros((rows, LANES), jnp.float32)
        for f in range(FIELDS):
            turn = (STRIP * f + side * STRIP) % LANES
            a = field(f, own_rows, cs_of(chunk))
            a = pltpu.roll(a, turn, 1) if turn else a
            strip = jnp.where(slot == f, a, strip)
        SP[side] = strip
    upper = lax.broadcasted_iota(jnp.int32, (8, cols), 0) >= 4
    inner = slice(LANES, LANES + cols)
    near = (slice(HALO + 8, HALO + 16), slice(HALO + rows - 16, HALO + rows - 8))
    for side in (0, 1):
        for t in range(PAIRS):
            a = field(2 * t, near[side], inner)
            if 2 * t + 1 < FIELDS:
                b = pltpu.roll(field(2 * t + 1, near[side], inner), 4, 0)
                a = jnp.where(upper, a, b) if side else jnp.where(upper, b, a)
            SR[side, t] = a
    for b in (-1, 1):
        side = (b + 1) // 2
        send(SP.at[side], RP.at[side, pl.ds(HALO, rows)], 0, b)
        for a in (-1, 1):
            src = pl.ds(0, HALO) if a < 0 else pl.ds(rows - HALO, HALO)
            dst = pl.ds(HALO + rows, HALO) if a < 0 else pl.ds(0, HALO)
            send(SP.at[side, src], RP.at[side, dst], a, b)
    for a in (-1, 1):
        side = (a + 1) // 2
        send(SR.at[side], RR.at[side], a, 0)
    for cp in sends:
        cp.wait_recv()

    every = slice(0, R)
    for side, chunk in ((0, NC - 1), (1, 0)):
        strip = RP[side]
        for f in range(FIELDS):
            turn = (-STRIP * f - side * STRIP) % LANES
            put(f, every, cs_of(chunk), pltpu.roll(strip, turn, 1) if turn else strip)
    far = (slice(R - 8, R), slice(0, 8))
    for side in (0, 1):
        for f in range(FIELDS):
            a = RR[side, f // 2]
            put(f, far[side], inner, pltpu.roll(a, 4, 0) if f % 2 else a)

    def shifts(read, n):
        lane = lax.broadcasted_iota(jnp.int32, (n, LANES), 1)
        first = lane == 0
        last = lane == LANES - 1
        memo = {}

        def get(kind, j):
            j = j % NC
            if (kind, j) not in memo:
                if kind == 0:
                    memo[kind, j] = read(j)
                else:
                    memo[kind, j] = pltpu.roll(get(0, j), 1 if kind < 0 else LANES - 1, 1)
            return memo[kind, j]

        def east(j):
            return jnp.where(last, get(1, j + 1), get(1, j))

        def west(j):
            return jnp.where(first, get(-1, j - 1), get(-1, j))

        return (lambda j: get(0, j)), east, west

    def north(a):
        return pltpu.roll(a, a.shape[0] - 1, 0)

    def south(a):
        return pltpu.roll(a, 1, 0)

    grow = lax.broadcasted_iota(jnp.int32, (R, LANES), 0) + (ilat * rows - HALO)
    keep = jnp.where((grow == nlat * rows - 1) | (grow == -1), 0.0, 1.0).astype(jnp.float32)

    mc, mE, mW = shifts(lambda j: M[:, cs_of(j)].astype(jnp.float32), R)
    for j in range(NC):
        m = mc(j)
        me = mE(j)
        mw = mW(j)
        mk = m * keep
        K[1][:, cs_of(j)] = C[0, :, cs_of(j)] * m * me
        K[6][:, cs_of(j)] = C[1, :, cs_of(j)] * mk * north(m)
        K[9][:, cs_of(j)] = C[2, :, cs_of(j)] * mk * north(me)
        K[10][:, cs_of(j)] = C[3, :, cs_of(j)] * mk * north(mw)
        VC[:, cs_of(j)] = B[:, cs_of(j)] * m

    cle, _, wle_of = shifts(lambda j: K[1][:, cs_of(j)], R)
    clne, _, wlne_of = shifts(lambda j: K[9][:, cs_of(j)], R)
    clnw, elnw_of, _ = shifts(lambda j: K[10][:, cs_of(j)], R)
    for j in range(NC):
        le = cle(j)
        wle = wle_of(j)
        ln = K[6][:, cs_of(j)]
        sln = south(ln)
        lne = clne(j)
        wlne = wlne_of(j)
        lnw = clnw(j)
        elnw = elnw_of(j)
        K[2][:, cs_of(j)] = wle
        K[3][:, cs_of(j)] = sln
        K[4][:, cs_of(j)] = south(lne)
        K[5][:, cs_of(j)] = south(lnw)
        K[7][:, cs_of(j)] = wlne
        K[8][:, cs_of(j)] = elnw
        d = E[:, cs_of(j)] + le + wle + ln + sln
        K[0][:, cs_of(j)] = d + lne + south(wlne) + lnw + south(elnw)

    theta, factors = level_factors()

    def apply(ref, rws, finish):
        n = rws.stop - rws.start
        centre, east, west = shifts(lambda j: ref[rws, cs_of(j)], n)
        for j in range(NC):
            v = centre(j)
            ve = east(j)
            vw = west(j)

            def k(i):
                return K[i][rws, cs_of(j)]

            p = k(3) * v + k(4) * ve + k(5) * vw
            q = k(6) * v + k(7) * vw + k(8) * ve
            finish(cs_of(j), v, k(0) * v - k(1) * ve - k(2) * vw - north(p) - south(q))

    mine = slice(HALO, HALO + rows)

    def round_of(it, rws):
        lo = HALO - rws.start

        def level0(cls, v, av):
            z = v * (1.0 / theta)
            step = factors[0][0] * z + factors[0][1] * (v - av * (1.0 / theta))
            S[rws, cls] = step
            Z[0][rws, cls] = z + step

        apply(VC, rws, level0)
        for level in range(1, DEG - 1):
            src = (level - 1) % 2

            def inner_level(cls, z, az):
                qq = VC[rws, cls] - az
                step = factors[level][0] * S[rws, cls] + factors[level][1] * qq
                new = z + step
                if level < DEG - 2:
                    S[rws, cls] = step
                    Z[1 - src][rws, cls] = new
                else:
                    UC[rws, cls] = new
                    U[it, :, cls] = new[lo : lo + rows]

            apply(Z[src], rws, inner_level)

        def last_level(cls, u, au):
            new = au - SHIFT * VC[rws, cls]
            VC[rws, cls] = new
            V[it + 1, :, cls] = new[lo : lo + rows]

        apply(UC, rws, last_level)

    for j in range(1, NC - 1):
        V[0, :, cs_of(j)] = VC[mine, cs_of(j)]
    round_of(0, slice(0, R))

    @pl.loop(1, ITERS)
    def _(it):
        round_of(it, slice(8, R - 8))

    hpairs = [((k + 1) // 2, k // 2) for k in range(2 * ITERS)]
    gpairs = [(k // 2, (k + 1) // 2) for k in range(2 * ITERS - 1)]

    def own(ref, n, j):
        return ref[n, :, cs_of(j)]

    def fold(a):
        return jnp.sum(a.reshape(rows // 8, 8, LANES), axis=0)

    def add(j, acc):
        v = [own(V, n, j) for n in range(ITERS + 1)]
        u = [own(U, n, j) for n in range(ITERS)]
        new = [fold(v[a] * u[b]) for a, b in hpairs] + [fold(v[a] * v[b]) for a, b in gpairs]
        return tuple(p + q for p, q in zip(acc, new))

    nsum = len(hpairs) + len(gpairs)
    acc = tuple(jnp.zeros((8, LANES), jnp.float32) for _ in range(nsum))
    for j in range(1, NC - 1):
        acc = add(j, acc)
    T2[...] = jnp.zeros_like(T2)
    for n, a in enumerate(acc):
        T2[n : n + 1, :] = jnp.sum(a, axis=0, keepdims=True)
    lo = T2[0:8, :]
    hi = T2[8:16, :]
    lo = lo + pltpu.roll(lo, LANES // 2, 1)
    hi = hi + pltpu.roll(hi, LANES // 2, 1)
    half = lax.broadcasted_iota(jnp.int32, (8, LANES), 1) < LANES // 2
    part = jnp.where(half, lo, hi)

    def exchange(part, slot, buf, axis, count, me, at, ssem, rsem):
        G[slot] = part
        buf[me] = part
        cps = []
        for d in range(1, count):
            cp = pltpu.make_async_remote_copy(
                src_ref=G.at[slot],
                dst_ref=buf.at[me],
                send_sem=ssem.at[d],
                recv_sem=rsem.at[d],
                device_id={axis: at(d)},
                device_id_type=MESH,
            )
            cp.start()
            cps.append(cp)
        for cp in cps:
            cp.wait_recv()
        total = buf[0]
        for n in range(1, count):
            total = total + buf[n]
        return total, cps

    total, c1 = exchange(part, 0, GL, "lat", nlat, ilat, lat_at, lat_s, lat_r)
    total, c2 = exchange(total, 1, GZ, "lon", nlon, ilon, lon_at, lon_s, lon_r)

    T_out[...] = total
    for cp in sends + c1 + c2:
        cp.wait_send()


def finish(V, U, T, x_out, r_out, n_out, XB, RB, T2, sems):
    total = T[...]
    rows, cols = XB.shape
    half = lax.broadcasted_iota(jnp.int32, (8, LANES), 1) < LANES // 2
    nh, ng = 2 * ITERS, 2 * ITERS - 1
    nsum = nh + ng
    for n, t in enumerate((jnp.where(half, total, 0.0), jnp.where(half, 0.0, total))):
        s = jnp.sum(t, axis=1, keepdims=True)
        T2[8 * n : 8 * n + 8, :] = jnp.broadcast_to(s, (8, LANES))
    sums = [T2[n : n + 1, :] for n in range(nsum)]
    xs, rs, norms = scalars(sums[:nh], sums[nh:])
    def cs_of(j):
        return slice(j * LANES, (j + 1) * LANES)
    cps = []
    for buf, out, co, src in ((XB, x_out, xs, U), (RB, r_out, rs, V)):
        for j in range(cols // LANES):
            x = co[0] * src[0, :, cs_of(j + 1)]
            for n in range(1, len(co)):
                x = x + co[n] * src[n, :, cs_of(j + 1)]
            buf[:, cs_of(j)] = x
        cp = pltpu.make_async_copy(buf, out, sems.at[len(cps)])
        cp.start()
        cps.append(cp)
    for n in range(ITERS):
        n_out[n] = norms[n][0, 0]
    for cp in cps:
        cp.wait()


def solution(mesh):
    nlat = mesh.shape["lat"]
    nlon = mesh.shape["lon"]

    def body(right_side, coefficients, extra, land_mask):
        rows, cols = right_side.shape
        R, W = rows + 2 * HALO, cols + 2 * LANES
        f32 = jnp.float32
        right_side, coefficients, extra, land_mask = (pltpu.with_memory_space_constraint(x, pltpu.HBM) for x in (right_side, coefficients, extra, land_mask))
        V, U, T = pl.pallas_call(
            functools.partial(kernel, nlat, nlon),
            out_shape=(
                pltpu.VMEM((ITERS + 1, rows, W), f32),
                pltpu.VMEM((ITERS, rows, W), f32),
                pltpu.VMEM((8, LANES), f32),
            ),
            in_specs=[pl.BlockSpec(memory_space=pl.ANY)] * 4,
            out_specs=(
                pl.BlockSpec(memory_space=pltpu.VMEM),
                pl.BlockSpec(memory_space=pltpu.VMEM),
                pl.BlockSpec(memory_space=pltpu.VMEM),
            ),
            scratch_shapes=[
                pltpu.VMEM((R, W), f32),
                pltpu.VMEM((4, R, W), f32),
                pltpu.VMEM((R, W), f32),
                pltpu.VMEM((R, W), jnp.int32),
                [pltpu.VMEM((R, W), f32)] * 11,
                pltpu.VMEM((R, W), f32),
                pltpu.VMEM((R, W), f32),
                pltpu.VMEM((R, W), f32),
                [pltpu.VMEM((R, W), f32)] * 2,
                pltpu.VMEM((2, rows, LANES), f32),
                pltpu.VMEM((2, R, LANES), f32),
                pltpu.VMEM((2, PAIRS, 8, cols), f32),
                pltpu.VMEM((2, PAIRS, 8, cols), f32),
                pltpu.VMEM((2, 8, LANES), f32),
                pltpu.VMEM((nlat, 8, LANES), f32),
                pltpu.VMEM((nlon, 8, LANES), f32),
                pltpu.VMEM((16, LANES), f32),
                pltpu.SemaphoreType.DMA((4,)),
                pltpu.SemaphoreType.DMA((16,)),
                pltpu.SemaphoreType.DMA((16,)),
                pltpu.SemaphoreType.DMA((nlat,)),
                pltpu.SemaphoreType.DMA((nlat,)),
                pltpu.SemaphoreType.DMA((nlon,)),
                pltpu.SemaphoreType.DMA((nlon,)),
            ],
            compiler_params=pltpu.CompilerParams(
                collective_id=0, has_side_effects=True, vmem_limit_bytes=VMEM_GRANT
            ),
        )(right_side, coefficients, extra, land_mask)
        return pl.pallas_call(
            finish,
            out_shape=(
                jax.ShapeDtypeStruct((rows, cols), f32),
                jax.ShapeDtypeStruct((rows, cols), f32),
                jax.ShapeDtypeStruct((ITERS,), f32),
            ),
            in_specs=[pl.BlockSpec(memory_space=pltpu.VMEM)] * 3,
            out_specs=(
                pl.BlockSpec(memory_space=pl.ANY),
                pl.BlockSpec(memory_space=pl.ANY),
                pl.BlockSpec(memory_space=pltpu.SMEM),
            ),
            scratch_shapes=[
                pltpu.VMEM((rows, cols), f32),
                pltpu.VMEM((rows, cols), f32),
                pltpu.VMEM((16, LANES), f32),
                pltpu.SemaphoreType.DMA((2,)),
            ],
            compiler_params=pltpu.CompilerParams(vmem_limit_bytes=4 * 1024 * 1024),
        )(V, U, T)

    return jax.shard_map(
        body,
        mesh=mesh,
        in_specs=(P("lat", "lon"), P(None, "lat", "lon"), P("lat", "lon"), P("lat", "lon")),
        out_specs=(P("lat", "lon"), P("lat", "lon"), P()),
        check_vma=False,
    )
```

```python
import functools

import jax
import jax.numpy as jnp
from jax import lax
from jax.experimental import pallas as pl
from jax.experimental.pallas import tpu as pltpu
from jax.sharding import PartitionSpec as P

DEG = 4
ITERS = 3
LOW_EIG = 0.25
HIGH_EIG = 20.5
SHIFT = 0.8
LANES = 128
TILE = 8
HALF = 4
STRIP = 16
FIELDS = 7
NGROUPS = 2
ALL_TO_ALL = 64
VMEM_GRANT = 24 * 1024 * 1024
FINISH_GRANT = 4 * 1024 * 1024
MESH = pl.DeviceIdType.MESH


def level_factors():
    theta = (HIGH_EIG + LOW_EIG) / 2.0
    delta = (HIGH_EIG - LOW_EIG) / 2.0
    sigma = theta / delta
    rho = 1.0 / sigma
    out = []
    for _ in range(DEG - 1):
        rho_new = 1.0 / (2.0 * sigma - rho)
        out.append((rho_new * rho, 2.0 * rho_new / delta))
        rho = rho_new
    return theta, out


def scalars(h, g):
    c = SHIFT
    ht = [h[k + 1] + c * h[k] for k in range(len(h) - 1)]

    def form(a, t):
        total = None
        for k in range(2 * len(a) - 1):
            pairs = None
            for i in range(len(a)):
                j = k - i
                if 0 <= j < len(a) and i <= j:
                    term = a[i] * a[j]
                    if i != j:
                        term = term + term
                    pairs = term if pairs is None else pairs + term
            pairs = pairs * t[k]
            total = pairs if total is None else total + pairs
        return total

    one = jnp.ones_like(h[0])
    zero = jnp.zeros_like(h[0])
    a = [one]
    b = [one]
    gamma = h[0]
    norms = [g[0]]
    alpha = gamma / ht[0]
    x = [zero] * ITERS
    beta = zero
    for k in range(ITERS):
        if k > 0:
            b = [a[i] + (beta * b[i] if i < len(b) else 0.0) for i in range(len(a))]
        for i in range(len(b)):
            x[i] = x[i] + alpha * b[i]
        tb = [
            (b[i - 1] if i > 0 else zero) + (c * b[i] if i < len(b) else zero)
            for i in range(len(b) + 1)
        ]
        a = [(a[i] if i < len(a) else zero) - alpha * tb[i] for i in range(len(tb))]
        if k < ITERS - 1:
            gamma_new = form(a, h)
            dlt = form(a, ht)
            norms.append(form(a, g))
            beta = gamma_new / gamma
            alpha = gamma_new / (dlt - beta * gamma_new / alpha)
            gamma = gamma_new
    return x, a, norms


HPAIRS = [((k + 1) // 2, k // 2) for k in range(2 * ITERS)]
GPAIRS = [(k // 2, (k + 1) // 2) for k in range(2 * ITERS - 1)]
NSUM = len(HPAIRS) + len(GPAIRS)


def cs_of(j):
    return slice(j * LANES, (j + 1) * LANES)


def ts_of(i):
    return slice(i * TILE, (i + 1) * TILE)


def groups_of(nc, count):
    if count == 1:
        return [(0, nc)], [list(range(nc + 1))]
    edges = [-(-nc * g // count) for g in range(count + 1)]
    spans = [(edges[g], edges[g + 1]) for g in range(count)]
    lists = []
    for g, (lo, hi) in enumerate(spans):
        own = list(range(lo, hi))
        own = [nc] + own if g == 0 else [lo - 1] + own
        lists.append(own + [nc] if g == count - 1 else own)
    return spans, lists


def kernel(
    nlat, nlon, rhs_in, coef_in, extra_in, mask_in, V, U, T_out,
    C, E, B, M, HC, HE, HB, HM, SR, RR, SP, RP, CP, K, L2, VC, S, Z, GS, G, G2,
    loc_sem, snd, rcv, red_s, red_r, ready,
):
    rows, cols = rhs_in.shape
    nr = rows // TILE
    nc = cols // LANES
    depth = ITERS
    ilat = lax.axis_index("lat")
    ilon = lax.axis_index("lon")
    has_n = ilat < nlat - 1
    has_s = ilat > 0

    local = [
        pltpu.make_async_copy(coef_in, C, loc_sem.at[0]),
        pltpu.make_async_copy(mask_in, M, loc_sem.at[1]),
        pltpu.make_async_copy(extra_in, E, loc_sem.at[2]),
        pltpu.make_async_copy(rhs_in, B, loc_sem.at[3]),
    ]
    for cp in local:
        cp.start()

    def lat_at(d):
        return lax.rem(ilat + d + nlat, nlat)

    def lon_at(d):
        return lax.rem(ilon + d + nlon, nlon)

    def where_to(a, b):
        out = {}
        if a:
            out["lat"] = lat_at(a)
        if b:
            out["lon"] = lon_at(b)
        return out

    barrier = pltpu.get_barrier_semaphore()

    def greet(sem, a, b):
        pl.semaphore_signal(sem, inc=1, device_id=where_to(a, b), device_id_type=MESH)

    for d in range(1, nlat):
        greet(barrier, d, 0)
    for d in range(1, nlon):
        greet(barrier, 0, d)
    for a, there in ((-1, has_s), (1, has_n)):

        @pl.when(there)
        def _():
            greet(barrier, a, -1)
            greet(barrier, a, 1)

    for side, there in ((0, has_n), (1, has_s)):

        @pl.when(jnp.logical_not(there))
        def _():
            for ref in (HC, HE, HB, HM, RR):
                ref[side] = jnp.zeros(ref.shape[1:], ref.dtype)
            for e in (0, 1):
                CP[e, side] = jnp.zeros(CP.shape[2:], jnp.float32)

    for cp in local:
        cp.wait()

    def own_field(f, rws, cls):
        if f < 4:
            return C[f, rws, cls]
        if f == 4:
            return E[rws, cls]
        if f == 5:
            return B[rws, cls]
        return M[rws, cls].astype(jnp.float32)

    sub = lax.broadcasted_iota(jnp.int32, (TILE, LANES), 0)
    lane = lax.broadcasted_iota(jnp.int32, (TILE, LANES), 1)
    slot = lane // STRIP
    for side, chunk in ((0, 0), (1, nc - 1)):
        for i in range(nr):
            strip = jnp.zeros((TILE, LANES), jnp.float32)
            for f in range(FIELDS):
                turn = (STRIP * f + side * STRIP) % LANES
                a = own_field(f, ts_of(i), cs_of(chunk))
                a = pltpu.roll(a, turn, 1) if turn else a
                strip = jnp.where(slot == f, a, strip)
            SP[side, ts_of(i), :] = strip
    far = (slice(TILE, TILE + HALF), slice(rows - TILE - HALF, rows - TILE))
    for side in (0, 1):
        for f in range(FIELDS):
            SR[side, f] = own_field(f, far[side], slice(0, cols))

    count = nlat - 1 + nlon - 1 + 2 * (has_n.astype(jnp.int32) + has_s.astype(jnp.int32))
    pl.semaphore_wait(barrier, count)
    direct = nlat * nlon <= ALL_TO_ALL
    if direct:
        for d in range(1, nlon):
            greet(ready, 0, d)

    sends = []

    def send(src, dst, a, b, stage):
        i = len(sends)
        cp = pltpu.make_async_remote_copy(
            src_ref=src, dst_ref=dst, send_sem=snd.at[i], recv_sem=rcv.at[i],
            device_id=where_to(a, b), device_id_type=MESH,
        )
        sends.append((cp, a, stage))
        return cp

    def each(cps, a, sending, act):
        def run():
            for cp in cps:
                act(cp)

        if a == 0:
            run()
        elif cps:
            pl.when((has_s if a < 0 else has_n) if sending else (has_n if a < 0 else has_s))(run)

    def start(cps, a):
        each(cps, a, True, lambda cp: cp.start())

    spans, lists = groups_of(nc, NGROUPS)
    start([send(SP.at[(b + 1) // 2], RP.at[(b + 1) // 2], 0, b, 0) for b in (-1, 1)], 0)
    for a in (-1, 1):
        side = (a + 1) // 2
        src = pl.ds(0, STRIP) if a < 0 else pl.ds(rows - STRIP, STRIP)
        start([send(SP.at[e, src], CP.at[e, side], a, 2 * e - 1, 0) for e in (0, 1)], a)
    for g, (lo, hi) in enumerate(spans):
        cl = pl.ds(lo * LANES, (hi - lo) * LANES)
        for a in (-1, 1):
            side = (a + 1) // 2
            edge = pl.ds(0, TILE) if a < 0 else pl.ds(rows - TILE, TILE)
            cps = [send(C.at[:, edge, cl], HC.at[side, :, :, cl], a, 0, g)]
            cps.append(send(M.at[edge, cl], HM.at[side, :, cl], a, 0, g))
            cps.append(send(E.at[edge, cl], HE.at[side, :, cl], a, 0, g))
            cps.append(send(B.at[edge, cl], HB.at[side, :, cl], a, 0, g))
            cps.append(send(SR.at[side, :, :, cl], RR.at[side, :, :, cl], a, 0, g))
            start(cps, a)

    up = sub < HALF
    s0 = sub == 0
    s3 = sub == HALF - 1
    s4 = sub == HALF
    s7 = sub == TILE - 1
    first = lane == 0
    last = lane == LANES - 1
    rim = (lane < STRIP) | (lane >= LANES - STRIP)

    def roll0(a, n):
        return pltpu.roll(a, n, 0)

    def halo_field(f, side, cls):
        if f < 4:
            return HC[side, f, :, cls]
        if f == 4:
            return HE[side, :, cls]
        if f == 5:
            return HB[side, :, cls]
        return HM[side, :, cls].astype(jnp.float32)

    def onion(n8, s8):
        near = jnp.where(up, n8, s8)
        return [near, jnp.where(up, roll0(n8, HALF), roll0(s8, HALF))]

    def raw(f, j):
        if j < nc:
            tiles = [own_field(f, ts_of(i), cs_of(j)) for i in range(nr)]
            tiles += onion(halo_field(f, 0, cs_of(j)), halo_field(f, 1, cs_of(j)))
            outer = [RR[side, f, :, cs_of(j)] for side in (0, 1)]
            return tiles + [jnp.concatenate(outer, axis=0)]

        def turned(read):
            out = []
            for e in (0, 1):
                turn = (-STRIP * f - e * STRIP) % LANES
                a = read(e)
                out.append(pltpu.roll(a, turn, 1) if turn else a)
            return jnp.where(lane < LANES // 2, out[0], out[1])

        tiles = [turned(lambda e, i=i: RP[e, ts_of(i), :]) for i in range(nr)]
        n8, n16 = (turned(lambda e, i=i: CP[e, 0, ts_of(i), :]) for i in (0, 1))
        s16, s8 = (turned(lambda e, i=i: CP[e, 1, ts_of(i), :]) for i in (0, 1))
        tiles = tiles + onion(n8, s8) + [jnp.where(up, n16, s16)]
        return [jnp.where(rim, t, 0.0) for t in tiles] if f == 6 else tiles

    def north(t, n):
        memo = {}

        def r3(i):
            if i not in memo:
                memo[i] = roll0(t[i], HALF - 1)
            return memo[i]

        r7 = [roll0(a, TILE - 1) for a in t]
        out = []
        for i in range(n):
            if i < nr:
                out.append(jnp.where(s7, r7[i + 1], r7[i]))
                continue
            a = jnp.where(s7, r7[0] if i == nr else r3(i - 1), r7[i])
            out.append(jnp.where(s3, r3(i + 1), a) if i + 1 < len(t) else a)
        return out

    def south(t, n):
        memo = {}

        def r5(i):
            if i not in memo:
                memo[i] = roll0(t[i], HALF + 1)
            return memo[i]

        r1 = [roll0(a, 1) for a in t]
        out = []
        for i in range(n):
            if i < nr:
                out.append(jnp.where(s0, r1[i - 1] if i else r1[nr], r1[i]))
                continue
            a = jnp.where(s0, r1[nr - 1] if i == nr else r5(i - 1), r1[i])
            out.append(jnp.where(s4, r5(i + 1), a) if i + 1 < len(t) else a)
        return out

    def shifts(read, order, ring):
        memo = {}

        def get(kind, p):
            p = p % len(order)
            if (kind, p) not in memo:
                if kind == 0:
                    memo[kind, p] = read(order[p])
                else:
                    turn = 1 if kind < 0 else LANES - 1
                    memo[kind, p] = [pltpu.roll(a, turn, 1) for a in get(0, p)]
            return memo[kind, p]

        def east(p):
            if p + 1 == len(order) and not ring:
                return get(1, p)
            return [jnp.where(last, b, a) for a, b in zip(get(1, p), get(1, p + 1))]

        def west(p):
            if p == 0 and not ring:
                return get(-1, p)
            return [jnp.where(first, b, a) for a, b in zip(get(-1, p), get(-1, p - 1))]

        return (lambda p: get(0, p)), east, west

    full = nr + depth

    def put(ref, k, j, tiles):
        for i, t in enumerate(tiles):
            ref[k, ts_of(i), cs_of(j)] = t

    def links(order, ring):
        mc, me_of, mw_of = shifts(lambda j: raw(6, j), order, ring)
        for p, j in enumerate(order):
            m, me, mw = mc(p), me_of(p), mw_of(p)
            nm, nme, nmw = north(m, full), north(me, full), north(mw, full)
            for k, f, o in ((1, 0, me), (6, 1, nm)):
                put(K, k, j, [c * a * b for c, a, b in zip(raw(f, j), m, o)])
            for k, f, o in ((0, 2, nme), (1, 3, nmw)):
                put(L2, k, j, [c * a * b for c, a, b in zip(raw(f, j), m, o)])
            for i, (a, b) in enumerate(zip(m, raw(5, j))):
                VC[ts_of(i), cs_of(j)] = a * b

        def tiles_of(ref, k):
            return lambda j: [ref[k, ts_of(i), cs_of(j)] for i in range(full)]

        cle, _, wle_of = shifts(tiles_of(K, 1), order, ring)
        clne, _, wlne_of = shifts(tiles_of(L2, 0), order, ring)
        clnw, elnw_of, _ = shifts(tiles_of(L2, 1), order, ring)
        for p, j in enumerate(order):
            le, wle, lne, wlne = cle(p), wle_of(p), clne(p), wlne_of(p)
            lnw, elnw = clnw(p), elnw_of(p)
            ln = tiles_of(K, 6)(j)
            sln = south(ln, full)
            swlne, selnw = south(wlne, full), south(elnw, full)
            put(K, 2, j, wle)
            put(K, 3, j, sln)
            put(K, 4, j, south(lne, full))
            put(K, 5, j, south(lnw, full))
            put(K, 7, j, wlne)
            put(K, 8, j, elnw)
            for i, d in enumerate(raw(4, j)):
                d = d + le[i] + wle[i] + ln[i] + sln[i]
                K[0, ts_of(i), cs_of(j)] = d + lne[i] + swlne[i] + lnw[i] + selnw[i]

    def apply(order, ring, ref, n_in, n_out, finish):
        centre, east, west = shifts(
            lambda j: [ref[ts_of(i), cs_of(j)] for i in range(n_in)], order, ring
        )
        used = min(n_in, n_out + 1)
        for p, j in enumerate(order):
            v, ve, vw = centre(p), east(p), west(p)

            def k(n, i):
                return K[n, ts_of(i), cs_of(j)]

            up_part = [k(3, i) * v[i] + k(4, i) * ve[i] + k(5, i) * vw[i] for i in range(used)]
            low_part = [k(6, i) * v[i] + k(7, i) * vw[i] + k(8, i) * ve[i] for i in range(used)]
            np_ = north(up_part, n_out)
            sq = south(low_part, n_out)
            for i in range(n_out):
                a = k(0, i) * v[i] - k(1, i) * ve[i] - k(2, i) * vw[i] - np_[i] - sq[i]
                finish(i, j, v[i], a)

    theta, factors = level_factors()
    seen = set()

    def record(ref, n, i, j, value):
        if i >= nr or j == nc:
            return
        if j in seen:
            value = jnp.where(lane < LANES // 2, ref[n, ts_of(i), cs_of(j)], value)
        ref[n, ts_of(i), cs_of(j)] = value

    def rounds(order, ring):
        for j in order:
            for i in range(nr):
                record(V, 0, i, j, VC[ts_of(i), cs_of(j)])
        for it in range(ITERS):
            n = full - it

            def level0(i, j, v, av):
                z = v * (1.0 / theta)
                step = factors[0][0] * z + factors[0][1] * (v - av * (1.0 / theta))
                S[ts_of(i), cs_of(j)] = step
                Z[0, ts_of(i), cs_of(j)] = z + step

            apply(order, ring, VC, n, n, level0)
            for level in range(1, DEG - 1):
                src = (level - 1) % 2

                def inner_level(i, j, z, az):
                    at = (ts_of(i), cs_of(j))
                    step = factors[level][0] * S[at] + factors[level][1] * (VC[at] - az)
                    new = z + step
                    Z[1 - src, ts_of(i), cs_of(j)] = new
                    if level < DEG - 2:
                        S[at] = step
                    else:
                        record(U, it, i, j, new)

                apply(order, ring, Z.at[src], n, n, inner_level)

            def last_level(i, j, u, au):
                at = (ts_of(i), cs_of(j))
                new = au - SHIFT * VC[at]
                VC[at] = new
                record(V, it + 1, i, j, new)

            apply(order, ring, Z.at[(DEG - 2) % 2], n, n - 1, last_level)

    acc = [None] * NSUM
    waited = 0
    for g, order in enumerate(lists):
        for a in (0, -1, 1):
            cps = [cp for cp, d, stage in sends if d == a and stage == g]
            each(cps, a, False, lambda cp: cp.wait_recv())
        ring = len(lists) == 1
        links(order, ring)
        rounds(order, ring)
        done = [j for j in order if j < nc and (ring or g == len(lists) - 1 or j != order[-1])]
        for j in done:
            for i in range(nr):
                v = [V[n, ts_of(i), cs_of(j)] for n in range(ITERS + 1)]
                u = [U[n, ts_of(i), cs_of(j)] for n in range(ITERS)]
                new = [v[a] * u[b] for a, b in HPAIRS] + [v[a] * v[b] for a, b in GPAIRS]
                acc = [b if a is None else a + b for a, b in zip(acc, new)]
        seen.update(j for j in order if j < nc)

    row = jnp.zeros((TILE, LANES), jnp.float32)
    for n, a in enumerate(acc):
        row = jnp.where(lane == n, jnp.sum(a, axis=1, keepdims=True), row)
    row = jnp.sum(row, axis=0, keepdims=True)

    pending = []

    def gather(row, stage, buf, me, peers):
        GS[stage] = row
        buf[me] = row
        cps = []
        for a, b in peers:
            i = len(pending)
            cp = pltpu.make_async_remote_copy(
                src_ref=GS.at[stage], dst_ref=buf.at[me],
                send_sem=red_s.at[i], recv_sem=red_r.at[i],
                device_id=where_to(a, b), device_id_type=MESH,
            )
            cp.start()
            cps.append(cp)
            pending.append(cp)
        for cp in cps:
            cp.wait_recv()
        parts = [buf[n] for n in range(buf.shape[0])]
        while len(parts) > 1:
            odd = parts[len(parts) // 2 * 2 :]
            parts = [a + b for a, b in zip(parts[::2], parts[1::2])] + odd
        return parts[0]

    if direct:
        pl.semaphore_wait(ready, nlon - 1)
        peers = [(a, b) for a in range(nlat) for b in range(nlon) if a or b]
        row = gather(row, 0, G, ilat * nlon + ilon, peers)
    else:
        row = gather(row, 0, G, ilat, [(d, 0) for d in range(1, nlat)])
        row = gather(row, 1, G2, ilon, [(0, d) for d in range(1, nlon)])
    T_out[...] = jnp.broadcast_to(row, (TILE, LANES))

    for a in (0, -1, 1):
        cps = [cp for cp, d, _ in sends if d == a]
        each(cps, a, True, lambda cp: cp.wait_send())
    for cp in pending:
        cp.wait_send()


def finish(V, U, T, x_out, r_out, n_out, X, R, sems):
    rows, cols = X.shape
    total = T[...]
    sums = [jnp.broadcast_to(total[:, n : n + 1], (TILE, LANES)) for n in range(NSUM)]
    xs, rs, norms = scalars(sums[: len(HPAIRS)], sums[len(HPAIRS) :])
    cps = []
    for buf, out, co, src in ((X, x_out, xs, U), (R, r_out, rs, V)):
        for j in range(cols // LANES):
            for i in range(rows // TILE):
                at = (ts_of(i), cs_of(j))
                a = co[0] * src[0, ts_of(i), cs_of(j)]
                for n in range(1, len(co)):
                    a = a + co[n] * src[n, ts_of(i), cs_of(j)]
                buf[at] = a
        cp = pltpu.make_async_copy(buf, out, sems.at[len(cps)])
        cp.start()
        cps.append(cp)
    for n in range(ITERS):
        n_out[n] = norms[n][0, 0]
    for cp in cps:
        cp.wait()


def solution(mesh):
    nlat = mesh.shape["lat"]
    nlon = mesh.shape["lon"]

    def body(*args):
        rows, cols = args[0].shape
        nc = cols // LANES
        W = cols + LANES
        R = rows + ITERS * TILE
        f32, i32 = jnp.float32, jnp.int32
        ndev = nlat * nlon
        direct = ndev <= ALL_TO_ALL
        npeers = ndev - 1 if direct else nlat + nlon - 2
        nsend = 6 + 10 * NGROUPS
        vmem, dma = pltpu.VMEM, pltpu.SemaphoreType.DMA
        args = [pltpu.with_memory_space_constraint(a, pltpu.HBM) for a in args]
        V, U, T = pl.pallas_call(
            functools.partial(kernel, nlat, nlon),
            out_shape=(
                vmem((ITERS + 1, rows, cols), f32),
                vmem((ITERS, rows, cols), f32),
                vmem((TILE, LANES), f32),
            ),
            in_specs=[pl.BlockSpec(memory_space=pl.ANY)] * 4,
            out_specs=(pl.BlockSpec(memory_space=pltpu.VMEM),) * 3,
            scratch_shapes=[
                vmem((4, rows, cols), f32),
                vmem((rows, cols), f32),
                vmem((rows, cols), f32),
                vmem((rows, cols), i32),
                vmem((2, 4, TILE, cols), f32),
                vmem((2, TILE, cols), f32),
                vmem((2, TILE, cols), f32),
                vmem((2, TILE, cols), i32),
                vmem((2, FIELDS, HALF, cols), f32),
                vmem((2, FIELDS, HALF, cols), f32),
                vmem((2, rows, LANES), f32),
                vmem((2, rows, LANES), f32),
                vmem((2, 2, STRIP, LANES), f32),
                vmem((9, R, W), f32),
                vmem((2, R, W), f32),
                vmem((R, W), f32),
                vmem((R, W), f32),
                vmem((2, R, W), f32),
                vmem((2, 1, LANES), f32),
                vmem((ndev if direct else nlat, 1, LANES), f32),
                vmem((nlon, 1, LANES), f32),
                dma((4,)),
                dma((nsend,)),
                dma((nsend,)),
                dma((npeers,)),
                dma((npeers,)),
                pltpu.SemaphoreType.REGULAR,
            ],
            compiler_params=pltpu.CompilerParams(
                collective_id=0, has_side_effects=True, vmem_limit_bytes=VMEM_GRANT
            ),
        )(*args)
        return pl.pallas_call(
            finish,
            out_shape=(
                jax.ShapeDtypeStruct((rows, cols), f32),
                jax.ShapeDtypeStruct((rows, cols), f32),
                jax.ShapeDtypeStruct((ITERS,), f32),
            ),
            in_specs=[pl.BlockSpec(memory_space=pltpu.VMEM)] * 3,
            out_specs=(
                pl.BlockSpec(memory_space=pl.ANY),
                pl.BlockSpec(memory_space=pl.ANY),
                pl.BlockSpec(memory_space=pltpu.SMEM),
            ),
            scratch_shapes=[vmem((rows, cols), f32), vmem((rows, cols), f32), dma((2,))],
            compiler_params=pltpu.CompilerParams(vmem_limit_bytes=FINISH_GRANT),
        )(V, U, T)

    return jax.shard_map(
        body,
        mesh=mesh,
        in_specs=(P("lat", "lon"), P(None, "lat", "lon"), P("lat", "lon"), P("lat", "lon")),
        out_specs=(P("lat", "lon"), P("lat", "lon"), P()),
        check_vma=False,
    )
```

```python
import functools

import jax
import jax.numpy as jnp
from jax import lax
from jax.experimental import pallas as pl
from jax.experimental.pallas import tpu as pltpu
from jax.sharding import PartitionSpec as P

DEG = 4
ITERS = 3
LOW_EIG = 0.25
HIGH_EIG = 20.5
SHIFT = 0.8
LANES = 128
TILE = 8
HALF = 4
STRIP = 16
FIELDS = 7
NGROUPS = 2
ALL_TO_ALL = 64
VMEM_GRANT = 24 * 1024 * 1024
FINISH_GRANT = 4 * 1024 * 1024
MESH = pl.DeviceIdType.MESH


def factored():
    theta = (HIGH_EIG + LOW_EIG) / 2.0
    delta = (HIGH_EIG - LOW_EIG) / 2.0
    sigma = theta / delta
    rho = 1.0 / sigma
    step = at_zero = 1.0 / theta
    for _ in range(DEG - 1):
        rho_new = 1.0 / (2.0 * sigma - rho)
        step = rho_new * rho * step + 2.0 * rho_new / delta
        at_zero = at_zero + step
        rho = rho_new
    bump = theta * theta - delta * delta
    return theta, bump, at_zero / (-2.0 * theta * (theta * theta + bump))


def scalars(h, g):
    c = SHIFT
    ht = [h[k + 1] + c * h[k] for k in range(len(h) - 1)]

    def form(a, t):
        total = None
        for k in range(2 * len(a) - 1):
            pairs = None
            for i in range(len(a)):
                j = k - i
                if 0 <= j < len(a) and i <= j:
                    term = a[i] * a[j]
                    if i != j:
                        term = term + term
                    pairs = term if pairs is None else pairs + term
            pairs = pairs * t[k]
            total = pairs if total is None else total + pairs
        return total

    one = jnp.ones_like(h[0])
    zero = jnp.zeros_like(h[0])
    a = [one]
    b = [one]
    gamma = h[0]
    norms = [g[0]]
    alpha = gamma / ht[0]
    x = [zero] * ITERS
    beta = zero
    for k in range(ITERS):
        if k > 0:
            b = [a[i] + (beta * b[i] if i < len(b) else 0.0) for i in range(len(a))]
        for i in range(len(b)):
            x[i] = x[i] + alpha * b[i]
        tb = [
            (b[i - 1] if i > 0 else zero) + (c * b[i] if i < len(b) else zero)
            for i in range(len(b) + 1)
        ]
        a = [(a[i] if i < len(a) else zero) - alpha * tb[i] for i in range(len(tb))]
        if k < ITERS - 1:
            gamma_new = form(a, h)
            dlt = form(a, ht)
            norms.append(form(a, g))
            beta = gamma_new / gamma
            alpha = gamma_new / (dlt - beta * gamma_new / alpha)
            gamma = gamma_new
    return x, a, norms


HPAIRS = [((k + 1) // 2, k // 2) for k in range(2 * ITERS)]
GPAIRS = [(k // 2, (k + 1) // 2) for k in range(2 * ITERS - 1)]
NSUM = len(HPAIRS) + len(GPAIRS)


def cs_of(j):
    return slice(j * LANES, (j + 1) * LANES)


def ts_of(i):
    return slice(i * TILE, (i + 1) * TILE)


def groups_of(nc, count):
    if count == 1:
        return [(0, nc)], [list(range(nc + 1))]
    edges = [-(-nc * g // count) for g in range(count + 1)]
    spans = [(edges[g], edges[g + 1]) for g in range(count)]
    lists = []
    for g, (lo, hi) in enumerate(spans):
        own = list(range(lo, hi))
        own = [nc] + own if g == 0 else [lo - 1] + own
        lists.append(own + [nc] if g == count - 1 else own)
    return spans, lists


def kernel(
    nlat, nlon, rhs_in, coef_in, extra_in, mask_in, V, U, T_out,
    C, E, B, M, HC, HE, HB, HM, SR, RR, SP, RP, CP, K, L2, VC, Z, GS, G, G2,
    LC, LE, LB, LM, LR, loc_sem, snd, rcv, red_s, red_r, rel_s, rel_r, ready,
):
    rows, cols = rhs_in.shape
    nr = rows // TILE
    nc = cols // LANES
    depth = ITERS
    ilat = lax.axis_index("lat")
    ilon = lax.axis_index("lon")
    has_n = ilat < nlat - 1
    has_s = ilat > 0

    local = [
        pltpu.make_async_copy(coef_in, C, loc_sem.at[0]),
        pltpu.make_async_copy(mask_in, M, loc_sem.at[1]),
        pltpu.make_async_copy(extra_in, E, loc_sem.at[2]),
        pltpu.make_async_copy(rhs_in, B, loc_sem.at[3]),
    ]
    for cp in local:
        cp.start()

    def lat_at(d):
        return lax.rem(ilat + d + nlat, nlat)

    def lon_at(d):
        return lax.rem(ilon + d + nlon, nlon)

    def where_to(a, b):
        out = {}
        if a:
            out["lat"] = lat_at(a)
        if b:
            out["lon"] = lon_at(b)
        return out

    barrier = pltpu.get_barrier_semaphore()

    def greet(sem, a, b):
        pl.semaphore_signal(sem, inc=1, device_id=where_to(a, b), device_id_type=MESH)

    for d in range(1, nlat):
        greet(barrier, d, 0)
    for d in range(1, nlon):
        greet(barrier, 0, d)
    for a, there in ((-1, has_s), (1, has_n)):

        @pl.when(there)
        def _():
            greet(barrier, a, -1)
            greet(barrier, a, 1)

    for side, there in ((0, has_n), (1, has_s)):

        @pl.when(jnp.logical_not(there))
        def _():
            for ref in (HC, HE, HB, HM, RR):
                ref[side] = jnp.zeros(ref.shape[1:], ref.dtype)
            for e in (0, 1):
                CP[e, side] = jnp.zeros(CP.shape[2:], jnp.float32)

    for cp in local:
        cp.wait()

    def own_field(f, rws, cls):
        if f < 4:
            return C[f, rws, cls]
        if f == 4:
            return E[rws, cls]
        if f == 5:
            return B[rws, cls]
        return M[rws, cls].astype(jnp.float32)

    count = nlat - 1 + nlon - 1 + 2 * (has_n.astype(jnp.int32) + has_s.astype(jnp.int32))
    pl.semaphore_wait(barrier, count)
    direct = nlat * nlon <= ALL_TO_ALL
    if direct:
        for d in range(1, nlon):
            greet(ready, 0, d)

    sub = lax.broadcasted_iota(jnp.int32, (TILE, LANES), 0)
    lane = lax.broadcasted_iota(jnp.int32, (TILE, LANES), 1)
    slot = lane // STRIP
    sends = []
    relays = []
    mid = nlat // 2 - 1
    relaying = nlat % 2 == 0 and nlat >= 4
    at_mid = {1: ilat == mid, -1: ilat == mid + 1}
    at_relay = {1: ilat == nlat - 1, -1: ilat == 0}

    def send(src, dst, a, b, stage):
        i = len(sends)
        cp = pltpu.make_async_remote_copy(
            src_ref=src, dst_ref=dst, send_sem=snd.at[i], recv_sem=rcv.at[i],
            device_id=where_to(a, b), device_id_type=MESH,
        )
        sends.append((cp, a, stage))
        return cp

    def each(cps, a, sending, act):
        def run():
            for cp in cps:
                act(cp)

        if a == 0:
            run()
        elif cps:
            pl.when((has_s if a < 0 else has_n) if sending else (has_n if a < 0 else has_s))(run)

    def start(cps, a):
        each(cps, a, True, lambda cp: cp.start())

    def detour(src, via, dst, a, i):
        k = len(relays)
        ends = {1: (nlat - 1, mid + 1), -1: (0, mid)}[a]
        legs = [
            pltpu.make_async_remote_copy(
                src_ref=src, dst_ref=via, send_sem=snd.at[i], recv_sem=rel_r.at[k],
                device_id={"lat": ends[0]}, device_id_type=MESH,
            ),
            pltpu.make_async_remote_copy(
                src_ref=via, dst_ref=dst, send_sem=rel_s.at[k], recv_sem=rcv.at[i],
                device_id={"lat": ends[1]}, device_id_type=MESH,
            ),
        ]
        relays.append((legs, a))
        return legs

    spans, lists = groups_of(nc, NGROUPS)
    ng = len(spans)
    stage_of = (ng - 1, 0)
    for g, (lo, hi) in enumerate(spans):
        cl = pl.ds(lo * LANES, (hi - lo) * LANES)
        relayed = relaying and g == ng - 1
        batches = {}
        for a in (-1, 1):
            side = (a + 1) // 2
            edge = pl.ds(0, TILE) if a < 0 else pl.ds(rows - TILE, TILE)
            moves = [
                (C.at[:, edge, cl], LC, HC.at[side, :, :, cl]),
                (M.at[edge, cl], LM, HM.at[side, :, cl]),
                (E.at[edge, cl], LE, HE.at[side, :, cl]),
                (B.at[edge, cl], LB, HB.at[side, :, cl]),
                (SR.at[side, :, :, cl], LR, RR.at[side, :, :, cl]),
            ]
            base = len(sends)
            cps = [send(src, dst, a, 0, g) for src, _, dst in moves]
            legs = [detour(*move, a, base + n) for n, move in enumerate(moves)] if relayed else []
            batches[a] = (cps, legs)

        def launch(a, part):
            cps, legs = batches[a]
            if not legs:
                start(cps[part], a)
                return
            there = has_s if a < 0 else has_n

            @pl.when(there & jnp.logical_not(at_mid[a]))
            def _():
                for cp in cps[part]:
                    cp.start()

            @pl.when(at_mid[a])
            def _():
                for leg, _ in legs[part]:
                    leg.start()

        if g == 0:
            for a in (-1, 1):
                launch(a, slice(0, 4))
            for side, chunk in ((0, 0), (1, nc - 1)):
                for i in range(nr):
                    strip = jnp.zeros((TILE, LANES), jnp.float32)
                    for f in range(FIELDS):
                        turn = (STRIP * f + side * STRIP) % LANES
                        a = own_field(f, ts_of(i), cs_of(chunk))
                        a = pltpu.roll(a, turn, 1) if turn else a
                        strip = jnp.where(slot == f, a, strip)
                    SP[side, ts_of(i), :] = strip
            start([send(SP.at[e], RP.at[e], 0, 2 * e - 1, stage_of[e]) for e in (1, 0)], 0)
            far = (slice(TILE, TILE + HALF), slice(rows - TILE - HALF, rows - TILE))
            for side in (0, 1):
                for f in range(FIELDS):
                    SR[side, f] = own_field(f, far[side], slice(0, cols))
            for a in (-1, 1):
                launch(a, slice(4, 5))
        else:
            for a in (-1, 1):
                launch(a, slice(0, 5))
        for e in (0, 1):
            if stage_of[e] != g:
                continue
            for a in (-1, 1):
                src = pl.ds(0, STRIP) if a < 0 else pl.ds(rows - STRIP, STRIP)
                start([send(SP.at[e, src], CP.at[e, (a + 1) // 2], a, 2 * e - 1, g)], a)

    for a in (-1, 1):
        mine = [legs for legs, d in relays if d == a]
        if mine:

            @pl.when(at_relay[a])
            def _():
                for first, second in mine:
                    first.wait_recv()
                    second.start()

    up = sub < HALF
    s0 = sub == 0
    s3 = sub == HALF - 1
    s4 = sub == HALF
    s7 = sub == TILE - 1
    first = lane == 0
    last = lane == LANES - 1
    rims = (lane < STRIP, lane >= LANES - STRIP)

    def roll0(a, n):
        return pltpu.roll(a, n, 0)

    def halo_field(f, side, cls):
        if f < 4:
            return HC[side, f, :, cls]
        if f == 4:
            return HE[side, :, cls]
        if f == 5:
            return HB[side, :, cls]
        return HM[side, :, cls].astype(jnp.float32)

    def onion(n8, s8):
        near = jnp.where(up, n8, s8)
        return [near, jnp.where(up, roll0(n8, HALF), roll0(s8, HALF))]

    def raw(f, j, ends):
        if j < nc:
            tiles = [own_field(f, ts_of(i), cs_of(j)) for i in range(nr)]
            tiles += onion(halo_field(f, 0, cs_of(j)), halo_field(f, 1, cs_of(j)))
            outer = [RR[side, f, :, cs_of(j)] for side in (0, 1)]
            return tiles + [jnp.concatenate(outer, axis=0)]

        def turned(read):
            out = []
            for e in ends:
                turn = (-STRIP * f - e * STRIP) % LANES
                a = read(e)
                out.append(pltpu.roll(a, turn, 1) if turn else a)
            return jnp.where(lane < LANES // 2, out[0], out[1]) if len(out) > 1 else out[0]

        tiles = [turned(lambda e, i=i: RP[e, ts_of(i), :]) for i in range(nr)]
        n8, n16 = (turned(lambda e, i=i: CP[e, 0, ts_of(i), :]) for i in (0, 1))
        s16, s8 = (turned(lambda e, i=i: CP[e, 1, ts_of(i), :]) for i in (0, 1))
        tiles = tiles + onion(n8, s8) + [jnp.where(up, n16, s16)]
        if f < 6:
            return tiles
        rim = rims[ends[0]] if len(ends) == 1 else rims[0] | rims[1]
        return [jnp.where(rim, t, 0.0) for t in tiles]

    def north(t, n):
        memo = {}

        def r3(i):
            if i not in memo:
                memo[i] = roll0(t[i], HALF - 1)
            return memo[i]

        r7 = [roll0(a, TILE - 1) for a in t]
        out = []
        for i in range(n):
            if i < nr:
                out.append(jnp.where(s7, r7[i + 1], r7[i]))
                continue
            a = jnp.where(s7, r7[0] if i == nr else r3(i - 1), r7[i])
            out.append(jnp.where(s3, r3(i + 1), a) if i + 1 < len(t) else a)
        return out

    def south(t, n):
        memo = {}

        def r5(i):
            if i not in memo:
                memo[i] = roll0(t[i], HALF + 1)
            return memo[i]

        r1 = [roll0(a, 1) for a in t]
        out = []
        for i in range(n):
            if i < nr:
                out.append(jnp.where(s0, r1[i - 1] if i else r1[nr], r1[i]))
                continue
            a = jnp.where(s0, r1[nr - 1] if i == nr else r5(i - 1), r1[i])
            out.append(jnp.where(s4, r5(i + 1), a) if i + 1 < len(t) else a)
        return out

    def shifts(read, order, ring):
        memo = {}

        def get(kind, p):
            p = p % len(order)
            if (kind, p) not in memo:
                if kind == 0:
                    memo[kind, p] = read(order[p])
                else:
                    turn = 1 if kind < 0 else LANES - 1
                    memo[kind, p] = [pltpu.roll(a, turn, 1) for a in get(0, p)]
            return memo[kind, p]

        def east(p):
            if p + 1 == len(order) and not ring:
                return get(1, p)
            return [jnp.where(last, b, a) for a, b in zip(get(1, p), get(1, p + 1))]

        def west(p):
            if p == 0 and not ring:
                return get(-1, p)
            return [jnp.where(first, b, a) for a, b in zip(get(-1, p), get(-1, p - 1))]

        return (lambda p: get(0, p)), east, west

    full = nr + depth
    theta, bump, scale = factored()

    def put(ref, k, j, tiles):
        for i, t in enumerate(tiles):
            ref[k, ts_of(i), cs_of(j)] = t

    def links(order, ring, ends):
        mc, me_of, mw_of = shifts(lambda j: raw(6, j, ends), order, ring)
        for p, j in enumerate(order):
            m, me, mw = mc(p), me_of(p), mw_of(p)
            nm, nme, nmw = north(m, full), north(me, full), north(mw, full)
            for k, f, o in ((1, 0, me), (6, 1, nm)):
                put(K, k, j, [c * a * b for c, a, b in zip(raw(f, j, ends), m, o)])
            for k, f, o in ((0, 2, nme), (1, 3, nmw)):
                put(L2, k, j, [c * a * b for c, a, b in zip(raw(f, j, ends), m, o)])
            for i, (a, b) in enumerate(zip(m, raw(5, j, ends))):
                VC[ts_of(i), cs_of(j)] = a * b

        def tiles_of(ref, k):
            return lambda j: [ref[k, ts_of(i), cs_of(j)] for i in range(full)]

        cle, _, wle_of = shifts(tiles_of(K, 1), order, ring)
        clne, _, wlne_of = shifts(tiles_of(L2, 0), order, ring)
        clnw, elnw_of, _ = shifts(tiles_of(L2, 1), order, ring)
        for p, j in enumerate(order):
            le, wle, lne, wlne = cle(p), wle_of(p), clne(p), wlne_of(p)
            lnw, elnw = clnw(p), elnw_of(p)
            ln = tiles_of(K, 6)(j)
            sln = south(ln, full)
            swlne, selnw = south(wlne, full), south(elnw, full)
            put(K, 2, j, wle)
            put(K, 3, j, sln)
            put(K, 4, j, south(lne, full))
            put(K, 5, j, south(lnw, full))
            put(K, 7, j, wlne)
            put(K, 8, j, elnw)
            for i, d in enumerate(raw(4, j, ends)):
                d = d + le[i] + wle[i] + ln[i] + sln[i]
                d = d + lne[i] + swlne[i] + lnw[i] + selnw[i]
                K[0, ts_of(i), cs_of(j)] = d
                K[9, ts_of(i), cs_of(j)] = d - theta
                K[10, ts_of(i), cs_of(j)] = d - 2.0 * theta

    def apply(order, ring, ref, diag, n_in, n_out, finish, skip=()):
        centre, east, west = shifts(
            lambda j: [ref[ts_of(i), cs_of(j)] for i in range(n_in)], order, ring
        )
        used = min(n_in, n_out + 1)
        for p, j in enumerate(order):
            if j in skip:
                continue
            v, ve, vw = centre(p), east(p), west(p)

            def k(n, i):
                return K[n, ts_of(i), cs_of(j)]

            up_part = [k(3, i) * v[i] + k(4, i) * ve[i] + k(5, i) * vw[i] for i in range(used)]
            low_part = [k(6, i) * v[i] + k(7, i) * vw[i] + k(8, i) * ve[i] for i in range(used)]
            np_ = north(up_part, n_out)
            sq = south(low_part, n_out)
            for i in range(n_out):
                a = k(diag, i) * v[i] - k(1, i) * ve[i] - k(2, i) * vw[i] - np_[i] - sq[i]
                finish(i, j, a)

    seen = set()

    def record(ref, n, i, j, value):
        if i >= nr or j == nc:
            return
        if j in seen:
            value = jnp.where(lane < LANES // 2, ref[n, ts_of(i), cs_of(j)], value)
        ref[n, ts_of(i), cs_of(j)] = value

    def rounds(order, ring):
        for j in order:
            for i in range(nr):
                record(V, 0, i, j, VC[ts_of(i), cs_of(j)])
        for it in range(ITERS):
            n = full - it

            def level0(i, j, a):
                Z[0, ts_of(i), cs_of(j)] = a

            def level1(i, j, a):
                at = (ts_of(i), cs_of(j))
                Z[1, ts_of(i), cs_of(j)] = scale * a + (scale * bump) * VC[at]

            def level2(i, j, a):
                Z[0, ts_of(i), cs_of(j)] = a
                record(U, it, i, j, a)

            def last_level(i, j, a):
                at = (ts_of(i), cs_of(j))
                new = a - SHIFT * VC[at]
                if it < ITERS - 1:
                    VC[at] = new
                record(V, it + 1, i, j, new)

            apply(order, ring, VC, 9, n, n, level0)
            apply(order, ring, Z.at[0], 9, n, n, level1)
            apply(order, ring, Z.at[1], 10, n, n, level2)
            skip = (nc,) if it == ITERS - 1 else ()
            apply(order, ring, Z.at[0], 0, n, n - 1, last_level, skip)

    acc = [None] * NSUM
    waited = 0
    for g, order in enumerate(lists):
        for a in (0, -1, 1):
            cps = [cp for cp, d, stage in sends if d == a and stage == g]
            each(cps, a, False, lambda cp: cp.wait_recv())
        ring = len(lists) == 1
        links(order, ring, [e for e in (0, 1) if stage_of[e] == g])
        rounds(order, ring)
        done = [j for j in order if j < nc and (ring or g == len(lists) - 1 or j != order[-1])]
        for j in done:
            for i in range(nr):
                v = [V[n, ts_of(i), cs_of(j)] for n in range(ITERS + 1)]
                u = [U[n, ts_of(i), cs_of(j)] for n in range(ITERS)]
                new = [v[a] * u[b] for a, b in HPAIRS] + [v[a] * v[b] for a, b in GPAIRS]
                acc = [b if a is None else a + b for a, b in zip(acc, new)]
        seen.update(j for j in order if j < nc)

    row = jnp.zeros((TILE, LANES), jnp.float32)
    for n, a in enumerate(acc):
        row = jnp.where(lane == n, jnp.sum(a, axis=1, keepdims=True), row)
    row = jnp.sum(row, axis=0, keepdims=True)

    pending = []
    paired = nlat & (nlat - 1) == 0

    def peer(a, b):
        if not paired:
            return where_to(a, b)
        to, bit = ilat, 1
        while bit < nlat:
            if a & bit:
                to = to + bit - 2 * bit * (lax.div(ilat, bit) % 2)
            bit *= 2
        return {"lat": to, "lon": lon_at(b)}

    def drain():
        for a in (0, -1, 1):
            cps = [cp for cp, d, _ in sends if d == a]
            each(cps, a, True, lambda cp: cp.wait_send())
        for a in (-1, 1):
            mine = [legs for legs, d in relays if d == a]
            if mine:

                @pl.when(at_relay[a])
                def _():
                    for _, second in mine:
                        second.wait_send()

    def gather(row, stage, buf, me, peers):
        GS[stage] = row
        buf[me] = row
        cps = []
        for a, b in peers:
            i = len(pending)
            cp = pltpu.make_async_remote_copy(
                src_ref=GS.at[stage], dst_ref=buf.at[me],
                send_sem=red_s.at[i], recv_sem=red_r.at[i],
                device_id=peer(a, b), device_id_type=MESH,
            )
            cp.start()
            cps.append(cp)
            pending.append(cp)
        if stage == 0:
            drain()
        for cp in cps:
            cp.wait_send()
        for cp in cps[::-1]:
            cp.wait_recv()
        parts = [buf[n] for n in range(buf.shape[0])]
        while len(parts) > 1:
            odd = parts[len(parts) // 2 * 2 :]
            parts = [a + b for a, b in zip(parts[::2], parts[1::2])] + odd
        return parts[0]

    if direct:
        pl.semaphore_wait(ready, nlon - 1)
        peers = [(a, b) for a in range(nlat) for b in range(nlon) if a or b][::-1]
        row = gather(row, 0, G, ilat * nlon + ilon, peers)
    else:
        row = gather(row, 0, G, ilat, [(d, 0) for d in range(1, nlat)])
        row = gather(row, 1, G2, ilon, [(0, d) for d in range(1, nlon)])
    T_out[...] = jnp.broadcast_to(row, (TILE, LANES))


def finish(V, U, T, x_out, r_out, n_out, X, R, sems):
    rows, cols = X.shape
    total = T[...]
    sums = [jnp.broadcast_to(total[:, n : n + 1], (TILE, LANES)) for n in range(NSUM)]
    xs, rs, norms = scalars(sums[: len(HPAIRS)], sums[len(HPAIRS) :])
    cps = []
    for buf, out, co, src in ((X, x_out, xs, U), (R, r_out, rs, V)):
        for j in range(cols // LANES):
            for i in range(rows // TILE):
                at = (ts_of(i), cs_of(j))
                a = co[0] * src[0, ts_of(i), cs_of(j)]
                for n in range(1, len(co)):
                    a = a + co[n] * src[n, ts_of(i), cs_of(j)]
                buf[at] = a
        cp = pltpu.make_async_copy(buf, out, sems.at[len(cps)])
        cp.start()
        cps.append(cp)
    for n in range(ITERS):
        n_out[n] = norms[n][0, 0]
    for cp in cps:
        cp.wait()


def solution(mesh):
    nlat = mesh.shape["lat"]
    nlon = mesh.shape["lon"]

    def body(*args):
        rows, cols = args[0].shape
        nc = cols // LANES
        W = cols + LANES
        R = rows + ITERS * TILE
        f32, i32 = jnp.float32, jnp.int32
        ndev = nlat * nlon
        direct = ndev <= ALL_TO_ALL
        npeers = ndev - 1 if direct else nlat + nlon - 2
        nsend = 6 + 10 * NGROUPS
        lo, hi = groups_of(nc, NGROUPS)[0][-1]
        half = (hi - lo) * LANES
        vmem, dma = pltpu.VMEM, pltpu.SemaphoreType.DMA
        args = [pltpu.with_memory_space_constraint(a, pltpu.HBM) for a in args]
        V, U, T = pl.pallas_call(
            functools.partial(kernel, nlat, nlon),
            out_shape=(
                vmem((ITERS + 1, rows, cols), f32),
                vmem((ITERS, rows, cols), f32),
                vmem((TILE, LANES), f32),
            ),
            in_specs=[pl.BlockSpec(memory_space=pl.ANY)] * 4,
            out_specs=(pl.BlockSpec(memory_space=pltpu.VMEM),) * 3,
            scratch_shapes=[
                vmem((4, rows, cols), f32),
                vmem((rows, cols), f32),
                vmem((rows, cols), f32),
                vmem((rows, cols), i32),
                vmem((2, 4, TILE, cols), f32),
                vmem((2, TILE, cols), f32),
                vmem((2, TILE, cols), f32),
                vmem((2, TILE, cols), i32),
                vmem((2, FIELDS, HALF, cols), f32),
                vmem((2, FIELDS, HALF, cols), f32),
                vmem((2, rows, LANES), f32),
                vmem((2, rows, LANES), f32),
                vmem((2, 2, STRIP, LANES), f32),
                vmem((11, R, W), f32),
                vmem((2, R, W), f32),
                vmem((R, W), f32),
                vmem((2, R, W), f32),
                vmem((2, 1, LANES), f32),
                vmem((ndev if direct else nlat, 1, LANES), f32),
                vmem((nlon, 1, LANES), f32),
                vmem((4, TILE, half), f32),
                vmem((TILE, half), f32),
                vmem((TILE, half), f32),
                vmem((TILE, half), i32),
                vmem((FIELDS, HALF, half), f32),
                dma((4,)),
                dma((nsend,)),
                dma((nsend,)),
                dma((npeers,)),
                dma((npeers,)),
                dma((10,)),
                dma((10,)),
                pltpu.SemaphoreType.REGULAR,
            ],
            compiler_params=pltpu.CompilerParams(
                collective_id=0, has_side_effects=True, vmem_limit_bytes=VMEM_GRANT
            ),
        )(*args)
        return pl.pallas_call(
            finish,
            out_shape=(
                jax.ShapeDtypeStruct((rows, cols), f32),
                jax.ShapeDtypeStruct((rows, cols), f32),
                jax.ShapeDtypeStruct((ITERS,), f32),
            ),
            in_specs=[pl.BlockSpec(memory_space=pltpu.VMEM)] * 3,
            out_specs=(
                pl.BlockSpec(memory_space=pl.ANY),
                pl.BlockSpec(memory_space=pl.ANY),
                pl.BlockSpec(memory_space=pltpu.SMEM),
            ),
            scratch_shapes=[vmem((rows, cols), f32), vmem((rows, cols), f32), dma((2,))],
            compiler_params=pltpu.CompilerParams(vmem_limit_bytes=FINISH_GRANT),
        )(V, U, T)

    return jax.shard_map(
        body,
        mesh=mesh,
        in_specs=(P("lat", "lon"), P(None, "lat", "lon"), P("lat", "lon"), P("lat", "lon")),
        out_specs=(P("lat", "lon"), P("lat", "lon"), P()),
        check_vma=False,
    )
```

```python
import functools

import jax
import jax.numpy as jnp
from jax import lax
from jax.experimental import pallas as pl
from jax.experimental.pallas import tpu as pltpu
from jax.sharding import PartitionSpec as P

DEG = 4
ITERS = 3
LOW_EIG = 0.25
HIGH_EIG = 20.5
SHIFT = 0.8
LANES = 128
TILE = 8
HALF = 4
STRIP = 16
FIELDS = 7
NGROUPS = 2
ALL_TO_ALL = 64
VMEM_GRANT = 24 * 1024 * 1024
FINISH_GRANT = 4 * 1024 * 1024
MESH = pl.DeviceIdType.MESH


def factored():
    theta = (HIGH_EIG + LOW_EIG) / 2.0
    delta = (HIGH_EIG - LOW_EIG) / 2.0
    sigma = theta / delta
    rho = 1.0 / sigma
    step = at_zero = 1.0 / theta
    for _ in range(DEG - 1):
        rho_new = 1.0 / (2.0 * sigma - rho)
        step = rho_new * rho * step + 2.0 * rho_new / delta
        at_zero = at_zero + step
        rho = rho_new
    bump = theta * theta - delta * delta
    return theta, bump, at_zero / (-2.0 * theta * (theta * theta + bump))


def scalars(h, g):
    c = SHIFT
    ht = [h[k + 1] + c * h[k] for k in range(len(h) - 1)]

    def form(a, t):
        total = None
        for k in range(2 * len(a) - 1):
            pairs = None
            for i in range(len(a)):
                j = k - i
                if 0 <= j < len(a) and i <= j:
                    term = a[i] * a[j]
                    if i != j:
                        term = term + term
                    pairs = term if pairs is None else pairs + term
            pairs = pairs * t[k]
            total = pairs if total is None else total + pairs
        return total

    one = jnp.ones_like(h[0])
    zero = jnp.zeros_like(h[0])
    a = [one]
    b = [one]
    gamma = h[0]
    norms = [g[0]]
    alpha = gamma / ht[0]
    x = [zero] * ITERS
    beta = zero
    for k in range(ITERS):
        if k > 0:
            b = [a[i] + (beta * b[i] if i < len(b) else 0.0) for i in range(len(a))]
        for i in range(len(b)):
            x[i] = x[i] + alpha * b[i]
        tb = [
            (b[i - 1] if i > 0 else zero) + (c * b[i] if i < len(b) else zero)
            for i in range(len(b) + 1)
        ]
        a = [(a[i] if i < len(a) else zero) - alpha * tb[i] for i in range(len(tb))]
        if k < ITERS - 1:
            gamma_new = form(a, h)
            dlt = form(a, ht)
            norms.append(form(a, g))
            beta = gamma_new / gamma
            alpha = gamma_new / (dlt - beta * gamma_new / alpha)
            gamma = gamma_new
    return x, a, norms


HPAIRS = [((k + 1) // 2, k // 2) for k in range(2 * ITERS)]
GPAIRS = [(k // 2, (k + 1) // 2) for k in range(2 * ITERS - 1)]
NSUM = len(HPAIRS) + len(GPAIRS)


def cs_of(j):
    return slice(j * LANES, (j + 1) * LANES)


def ts_of(i):
    return slice(i * TILE, (i + 1) * TILE)


def groups_of(nc, count):
    if count == 1:
        return [(0, nc)], [list(range(nc + 1))]
    edges = [-(-nc * g // count) for g in range(count + 1)]
    spans = [(edges[g], edges[g + 1]) for g in range(count)]
    lists = []
    for g, (lo, hi) in enumerate(spans):
        own = list(range(lo, hi))
        own = [nc] + own if g == 0 else [lo - 1] + own
        lists.append(own + [nc] if g == count - 1 else own)
    return spans, lists


def kernel(
    nlat, nlon, rhs_in, coef_in, extra_in, mask_in, V, U, T_out,
    C, E, B, M, SR, RR, SP, RP, CP, K, L2, VC, Z, GS, G, G2,
    LR, loc_sem, snd, rcv, red_s, red_r, rel_s, rel_r, ready,
):
    rows, cols = rhs_in.shape
    nr = rows // TILE
    nc = cols // LANES
    depth = ITERS
    ilat = lax.axis_index("lat")
    ilon = lax.axis_index("lon")
    has_n = ilat < nlat - 1
    has_s = ilat > 0

    local = [
        pltpu.make_async_copy(coef_in, C, loc_sem.at[0]),
        pltpu.make_async_copy(mask_in, M, loc_sem.at[1]),
        pltpu.make_async_copy(extra_in, E, loc_sem.at[2]),
        pltpu.make_async_copy(rhs_in, B, loc_sem.at[3]),
    ]
    for cp in local:
        cp.start()

    def lat_at(d):
        return lax.rem(ilat + d + nlat, nlat)

    def lon_at(d):
        return lax.rem(ilon + d + nlon, nlon)

    def where_to(a, b):
        out = {}
        if a:
            out["lat"] = lat_at(a)
        if b:
            out["lon"] = lon_at(b)
        return out

    barrier = pltpu.get_barrier_semaphore()

    def greet(sem, a, b):
        pl.semaphore_signal(sem, inc=1, device_id=where_to(a, b), device_id_type=MESH)

    for d in range(1, nlat):
        greet(barrier, d, 0)
    for d in range(1, nlon):
        greet(barrier, 0, d)
    for a, there in ((-1, has_s), (1, has_n)):

        @pl.when(there)
        def _():
            greet(barrier, a, -1)
            greet(barrier, a, 1)

    for side, there in ((0, has_n), (1, has_s)):

        @pl.when(jnp.logical_not(there))
        def _():
            RR[side] = jnp.zeros(RR.shape[1:], jnp.float32)
            for e in (0, 1):
                CP[e, side] = jnp.zeros(CP.shape[2:], jnp.float32)

    for cp in local:
        cp.wait()

    def own_field(f, rws, cls):
        if f < 4:
            return C[f, rws, cls]
        if f == 4:
            return E[rws, cls]
        if f == 5:
            return B[rws, cls]
        return M[rws, cls].astype(jnp.float32)

    count = nlat - 1 + nlon - 1 + 2 * (has_n.astype(jnp.int32) + has_s.astype(jnp.int32))
    pl.semaphore_wait(barrier, count)
    direct = nlat * nlon <= ALL_TO_ALL
    if direct:
        for d in range(1, nlon):
            greet(ready, 0, d)

    sub = lax.broadcasted_iota(jnp.int32, (TILE, LANES), 0)
    lane = lax.broadcasted_iota(jnp.int32, (TILE, LANES), 1)
    slot = lane // STRIP
    sends = []
    relays = []
    mid = nlat // 2 - 1
    relaying = nlat % 2 == 0 and nlat >= 4
    at_mid = {1: ilat == mid, -1: ilat == mid + 1}
    at_relay = {1: ilat == nlat - 1, -1: ilat == 0}

    def send(src, dst, a, b, stage):
        i = len(sends)
        cp = pltpu.make_async_remote_copy(
            src_ref=src, dst_ref=dst, send_sem=snd.at[i], recv_sem=rcv.at[i],
            device_id=where_to(a, b), device_id_type=MESH,
        )
        sends.append((cp, a, stage))
        return cp

    def each(cps, a, sending, act):
        def run():
            for cp in cps:
                act(cp)

        if a == 0:
            run()
        elif cps:
            pl.when((has_s if a < 0 else has_n) if sending else (has_n if a < 0 else has_s))(run)

    def start(cps, a):
        each(cps, a, True, lambda cp: cp.start())

    def detour(src, via, dst, a, i):
        k = len(relays)
        ends = {1: (nlat - 1, mid + 1), -1: (0, mid)}[a]
        legs = [
            pltpu.make_async_remote_copy(
                src_ref=src, dst_ref=via, send_sem=snd.at[i], recv_sem=rel_r.at[k],
                device_id={"lat": ends[0]}, device_id_type=MESH,
            ),
            pltpu.make_async_remote_copy(
                src_ref=via, dst_ref=dst, send_sem=rel_s.at[k], recv_sem=rcv.at[i],
                device_id={"lat": ends[1]}, device_id_type=MESH,
            ),
        ]
        relays.append((legs, a))
        return legs

    spans, lists = groups_of(nc, NGROUPS)
    ng = len(spans)
    stage_of = (ng - 1, 0)

    def half_rows(side, k):
        first = k * HALF if side == 0 else rows - (k + 1) * HALF
        return slice(first, first + HALF)

    for g, (lo, hi) in enumerate(spans):
        for side in (0, 1):
            for f in range(FIELDS):
                for k in range(depth):
                    for j in range(lo, hi):
                        SR[side, f * depth + k, :, cs_of(j)] = own_field(f, half_rows(side, k), cs_of(j))
        cl = pl.ds(lo * LANES, (hi - lo) * LANES)
        for a in (-1, 1):
            side = (a + 1) // 2
            move = (SR.at[side, :, :, cl], LR, RR.at[side, :, :, cl])
            i = len(sends)
            cp = send(move[0], move[2], a, 0, g)
            if not (relaying and g == ng - 1):
                start([cp], a)
                continue
            leg = detour(*move, a, i)[0]
            there = has_s if a < 0 else has_n
            pl.when(there & jnp.logical_not(at_mid[a]))(lambda: cp.start())
            pl.when(at_mid[a])(lambda: leg.start())
        if g == 0:
            for side, chunk in ((0, 0), (1, nc - 1)):
                for i in range(nr):
                    strip = jnp.zeros((TILE, LANES), jnp.float32)
                    for f in range(FIELDS):
                        turn = (STRIP * f + side * STRIP) % LANES
                        a = own_field(f, ts_of(i), cs_of(chunk))
                        a = pltpu.roll(a, turn, 1) if turn else a
                        strip = jnp.where(slot == f, a, strip)
                    SP[side, ts_of(i), :] = strip
            start([send(SP.at[e], RP.at[e], 0, 2 * e - 1, stage_of[e]) for e in (1, 0)], 0)
        for e in (0, 1):
            if stage_of[e] != g:
                continue
            for a in (-1, 1):
                src = pl.ds(0, STRIP) if a < 0 else pl.ds(rows - STRIP, STRIP)
                start([send(SP.at[e, src], CP.at[e, (a + 1) // 2], a, 2 * e - 1, g)], a)

    for a in (-1, 1):
        mine = [legs for legs, d in relays if d == a]
        if mine:

            @pl.when(at_relay[a])
            def _():
                for first, second in mine:
                    first.wait_recv()
                    second.start()

    up = sub < HALF
    s0 = sub == 0
    s3 = sub == HALF - 1
    s4 = sub == HALF
    s7 = sub == TILE - 1
    first = lane == 0
    last = lane == LANES - 1
    rims = (lane < STRIP, lane >= LANES - STRIP)

    def roll0(a, n):
        return pltpu.roll(a, n, 0)

    def onion(n8, s8):
        near = jnp.where(up, n8, s8)
        return [near, jnp.where(up, roll0(n8, HALF), roll0(s8, HALF))]

    def raw(f, j, ends):
        if j < nc:
            tiles = [own_field(f, ts_of(i), cs_of(j)) for i in range(nr)]
            for k in range(depth):
                halves = [RR[side, f * depth + k, :, cs_of(j)] for side in (0, 1)]
                tiles.append(jnp.concatenate(halves, axis=0))
            return tiles

        def turned(read):
            out = []
            for e in ends:
                turn = (-STRIP * f - e * STRIP) % LANES
                a = read(e)
                out.append(pltpu.roll(a, turn, 1) if turn else a)
            return jnp.where(lane < LANES // 2, out[0], out[1]) if len(out) > 1 else out[0]

        tiles = [turned(lambda e, i=i: RP[e, ts_of(i), :]) for i in range(nr)]
        n8, n16 = (turned(lambda e, i=i: CP[e, 0, ts_of(i), :]) for i in (0, 1))
        s16, s8 = (turned(lambda e, i=i: CP[e, 1, ts_of(i), :]) for i in (0, 1))
        tiles = tiles + onion(n8, s8) + [jnp.where(up, n16, s16)]
        if f < 6:
            return tiles
        rim = rims[ends[0]] if len(ends) == 1 else rims[0] | rims[1]
        return [jnp.where(rim, t, 0.0) for t in tiles]

    def north(t, n):
        memo = {}

        def r3(i):
            if i not in memo:
                memo[i] = roll0(t[i], HALF - 1)
            return memo[i]

        r7 = [roll0(a, TILE - 1) for a in t]
        out = []
        for i in range(n):
            if i < nr:
                out.append(jnp.where(s7, r7[i + 1], r7[i]))
                continue
            a = jnp.where(s7, r7[0] if i == nr else r3(i - 1), r7[i])
            out.append(jnp.where(s3, r3(i + 1), a) if i + 1 < len(t) else a)
        return out

    def south(t, n):
        memo = {}

        def r5(i):
            if i not in memo:
                memo[i] = roll0(t[i], HALF + 1)
            return memo[i]

        r1 = [roll0(a, 1) for a in t]
        out = []
        for i in range(n):
            if i < nr:
                out.append(jnp.where(s0, r1[i - 1] if i else r1[nr], r1[i]))
                continue
            a = jnp.where(s0, r1[nr - 1] if i == nr else r5(i - 1), r1[i])
            out.append(jnp.where(s4, r5(i + 1), a) if i + 1 < len(t) else a)
        return out

    def shifts(read, order, ring):
        memo = {}

        def get(kind, p):
            p = p % len(order)
            if (kind, p) not in memo:
                if kind == 0:
                    memo[kind, p] = read(order[p])
                else:
                    turn = 1 if kind < 0 else LANES - 1
                    memo[kind, p] = [pltpu.roll(a, turn, 1) for a in get(0, p)]
            return memo[kind, p]

        def east(p):
            if p + 1 == len(order) and not ring:
                return get(1, p)
            return [jnp.where(last, b, a) for a, b in zip(get(1, p), get(1, p + 1))]

        def west(p):
            if p == 0 and not ring:
                return get(-1, p)
            return [jnp.where(first, b, a) for a, b in zip(get(-1, p), get(-1, p - 1))]

        return (lambda p: get(0, p)), east, west

    full = nr + depth
    theta, bump, scale = factored()

    def put(ref, k, j, tiles):
        for i, t in enumerate(tiles):
            ref[k, ts_of(i), cs_of(j)] = t

    def links(order, ring, ends):
        mc, me_of, mw_of = shifts(lambda j: raw(6, j, ends), order, ring)
        for p, j in enumerate(order):
            m, me, mw = mc(p), me_of(p), mw_of(p)
            nm, nme, nmw = north(m, full), north(me, full), north(mw, full)
            for k, f, o in ((1, 0, me), (6, 1, nm)):
                put(K, k, j, [c * a * b for c, a, b in zip(raw(f, j, ends), m, o)])
            for k, f, o in ((0, 2, nme), (1, 3, nmw)):
                put(L2, k, j, [c * a * b for c, a, b in zip(raw(f, j, ends), m, o)])
            for i, (a, b) in enumerate(zip(m, raw(5, j, ends))):
                VC[ts_of(i), cs_of(j)] = a * b

        def tiles_of(ref, k):
            return lambda j: [ref[k, ts_of(i), cs_of(j)] for i in range(full)]

        cle, _, wle_of = shifts(tiles_of(K, 1), order, ring)
        clne, _, wlne_of = shifts(tiles_of(L2, 0), order, ring)
        clnw, elnw_of, _ = shifts(tiles_of(L2, 1), order, ring)
        for p, j in enumerate(order):
            le, wle, lne, wlne = cle(p), wle_of(p), clne(p), wlne_of(p)
            lnw, elnw = clnw(p), elnw_of(p)
            ln = tiles_of(K, 6)(j)
            sln = south(ln, full)
            swlne, selnw = south(wlne, full), south(elnw, full)
            put(K, 2, j, wle)
            put(K, 3, j, sln)
            put(K, 4, j, south(lne, full))
            put(K, 5, j, south(lnw, full))
            put(K, 7, j, wlne)
            put(K, 8, j, elnw)
            for i, d in enumerate(raw(4, j, ends)):
                d = d + le[i] + wle[i] + ln[i] + sln[i]
                d = d + lne[i] + swlne[i] + lnw[i] + selnw[i]
                K[0, ts_of(i), cs_of(j)] = d
                K[9, ts_of(i), cs_of(j)] = d - theta
                K[10, ts_of(i), cs_of(j)] = d - 2.0 * theta

    def apply(order, ring, ref, diag, n_in, n_out, finish, skip=()):
        centre, east, west = shifts(
            lambda j: [ref[ts_of(i), cs_of(j)] for i in range(n_in)], order, ring
        )
        used = min(n_in, n_out + 1)
        for p, j in enumerate(order):
            if j in skip:
                continue
            v, ve, vw = centre(p), east(p), west(p)

            def k(n, i):
                return K[n, ts_of(i), cs_of(j)]

            up_part = [k(3, i) * v[i] + k(4, i) * ve[i] + k(5, i) * vw[i] for i in range(used)]
            low_part = [k(6, i) * v[i] + k(7, i) * vw[i] + k(8, i) * ve[i] for i in range(used)]
            np_ = north(up_part, n_out)
            sq = south(low_part, n_out)
            for i in range(n_out):
                a = k(diag, i) * v[i] - k(1, i) * ve[i] - k(2, i) * vw[i] - np_[i] - sq[i]
                finish(i, j, a)

    seen = set()

    def record(ref, n, i, j, value):
        if i >= nr or j == nc:
            return
        if j in seen:
            value = jnp.where(lane < LANES // 2, ref[n, ts_of(i), cs_of(j)], value)
        ref[n, ts_of(i), cs_of(j)] = value

    def rounds(order, ring):
        for j in order:
            for i in range(nr):
                record(V, 0, i, j, VC[ts_of(i), cs_of(j)])
        for it in range(ITERS):
            n = full - it

            def level0(i, j, a):
                Z[0, ts_of(i), cs_of(j)] = a

            def level1(i, j, a):
                at = (ts_of(i), cs_of(j))
                Z[1, ts_of(i), cs_of(j)] = scale * a + (scale * bump) * VC[at]

            def level2(i, j, a):
                Z[0, ts_of(i), cs_of(j)] = a
                record(U, it, i, j, a)

            def last_level(i, j, a):
                at = (ts_of(i), cs_of(j))
                new = a - SHIFT * VC[at]
                if it < ITERS - 1:
                    VC[at] = new
                record(V, it + 1, i, j, new)

            apply(order, ring, VC, 9, n, n, level0)
            apply(order, ring, Z.at[0], 9, n, n, level1)
            apply(order, ring, Z.at[1], 10, n, n, level2)
            skip = (nc,) if it == ITERS - 1 else ()
            apply(order, ring, Z.at[0], 0, n, n - 1, last_level, skip)

    acc = [None] * NSUM
    waited = 0
    for g, order in enumerate(lists):
        for a in (0, -1, 1):
            cps = [cp for cp, d, stage in sends if d == a and stage == g]
            each(cps, a, False, lambda cp: cp.wait_recv())
        ring = len(lists) == 1
        links(order, ring, [e for e in (0, 1) if stage_of[e] == g])
        rounds(order, ring)
        done = [j for j in order if j < nc and (ring or g == len(lists) - 1 or j != order[-1])]
        for j in done:
            for i in range(nr):
                v = [V[n, ts_of(i), cs_of(j)] for n in range(ITERS + 1)]
                u = [U[n, ts_of(i), cs_of(j)] for n in range(ITERS)]
                new = [v[a] * u[b] for a, b in HPAIRS] + [v[a] * v[b] for a, b in GPAIRS]
                acc = [b if a is None else a + b for a, b in zip(acc, new)]
        seen.update(j for j in order if j < nc)

    row = jnp.zeros((TILE, LANES), jnp.float32)
    for n, a in enumerate(acc):
        row = jnp.where(lane == n, jnp.sum(a, axis=1, keepdims=True), row)
    row = jnp.sum(row, axis=0, keepdims=True)

    pending = []
    paired = nlat & (nlat - 1) == 0

    def peer(a, b):
        if not paired:
            return where_to(a, b)
        to, bit = ilat, 1
        while bit < nlat:
            if a & bit:
                to = to + bit - 2 * bit * (lax.div(ilat, bit) % 2)
            bit *= 2
        return {"lat": to, "lon": lon_at(b)}

    def drain():
        for a in (0, -1, 1):
            cps = [cp for cp, d, _ in sends if d == a]
            each(cps, a, True, lambda cp: cp.wait_send())
        for a in (-1, 1):
            mine = [legs for legs, d in relays if d == a]
            if mine:

                @pl.when(at_relay[a])
                def _():
                    for _, second in mine:
                        second.wait_send()

    def gather(row, stage, buf, me, peers):
        GS[stage] = row
        buf[me] = row
        cps = []
        for a, b in peers:
            i = len(pending)
            cp = pltpu.make_async_remote_copy(
                src_ref=GS.at[stage], dst_ref=buf.at[me],
                send_sem=red_s.at[i], recv_sem=red_r.at[i],
                device_id=peer(a, b), device_id_type=MESH,
            )
            cp.start()
            cps.append(cp)
            pending.append(cp)
        if stage == 0:
            drain()
        for cp in cps:
            cp.wait_send()
        for cp in cps[::-1]:
            cp.wait_recv()
        parts = [buf[n] for n in range(buf.shape[0])]
        while len(parts) > 1:
            odd = parts[len(parts) // 2 * 2 :]
            parts = [a + b for a, b in zip(parts[::2], parts[1::2])] + odd
        return parts[0]

    if direct:
        pl.semaphore_wait(ready, nlon - 1)
        peers = [(a, b) for a in range(nlat) for b in range(nlon) if a or b][::-1]
        row = gather(row, 0, G, ilat * nlon + ilon, peers)
    else:
        row = gather(row, 0, G, ilat, [(d, 0) for d in range(1, nlat)])
        row = gather(row, 1, G2, ilon, [(0, d) for d in range(1, nlon)])
    T_out[...] = jnp.broadcast_to(row, (TILE, LANES))


def finish(V, U, T, x_out, r_out, n_out, X, R, N, sems):
    rows, cols = X.shape
    total = T[...]
    sums = [jnp.broadcast_to(total[:, n : n + 1], (TILE, LANES)) for n in range(NSUM)]
    xs, rs, norms = scalars(sums[: len(HPAIRS)], sums[len(HPAIRS) :])
    for n in range(ITERS):
        N[n] = norms[n][0, 0]
    cps = [pltpu.make_async_copy(N, n_out, sems.at[0])]
    cps[0].start()
    for buf, out, co, src in ((X, x_out, xs, U), (R, r_out, rs, V)):
        for j in range(cols // LANES):
            for i in range(rows // TILE):
                at = (ts_of(i), cs_of(j))
                a = co[0] * src[0, ts_of(i), cs_of(j)]
                for n in range(1, len(co)):
                    a = a + co[n] * src[n, ts_of(i), cs_of(j)]
                buf[at] = a
        cp = pltpu.make_async_copy(buf, out, sems.at[len(cps)])
        cp.start()
        cps.append(cp)
    for cp in cps:
        cp.wait()


def solution(mesh):
    nlat = mesh.shape["lat"]
    nlon = mesh.shape["lon"]

    def body(*args):
        rows, cols = args[0].shape
        nc = cols // LANES
        W = cols + LANES
        R = rows + ITERS * TILE
        f32, i32 = jnp.float32, jnp.int32
        ndev = nlat * nlon
        direct = ndev <= ALL_TO_ALL
        npeers = ndev - 1 if direct else nlat + nlon - 2
        nsend = 6 + 2 * NGROUPS
        lo, hi = groups_of(nc, NGROUPS)[0][-1]
        half = (hi - lo) * LANES
        vmem, dma = pltpu.VMEM, pltpu.SemaphoreType.DMA
        args = [pltpu.with_memory_space_constraint(a, pltpu.HBM) for a in args]
        V, U, T = pl.pallas_call(
            functools.partial(kernel, nlat, nlon),
            out_shape=(
                vmem((ITERS + 1, rows, cols), f32),
                vmem((ITERS, rows, cols), f32),
                vmem((TILE, LANES), f32),
            ),
            in_specs=[pl.BlockSpec(memory_space=pl.ANY)] * 4,
            out_specs=(pl.BlockSpec(memory_space=pltpu.VMEM),) * 3,
            scratch_shapes=[
                vmem((4, rows, cols), f32),
                vmem((rows, cols), f32),
                vmem((rows, cols), f32),
                vmem((rows, cols), i32),
                vmem((2, FIELDS * ITERS, HALF, cols), f32),
                vmem((2, FIELDS * ITERS, HALF, cols), f32),
                vmem((2, rows, LANES), f32),
                vmem((2, rows, LANES), f32),
                vmem((2, 2, STRIP, LANES), f32),
                vmem((11, R, W), f32),
                vmem((2, R, W), f32),
                vmem((R, W), f32),
                vmem((2, R, W), f32),
                vmem((2, 1, LANES), f32),
                vmem((ndev if direct else nlat, 1, LANES), f32),
                vmem((nlon, 1, LANES), f32),
                vmem((FIELDS * ITERS, HALF, half), f32),
                dma((4,)),
                dma((nsend,)),
                dma((nsend,)),
                dma((npeers,)),
                dma((npeers,)),
                dma((2,)),
                dma((2,)),
                pltpu.SemaphoreType.REGULAR,
            ],
            compiler_params=pltpu.CompilerParams(
                collective_id=0, has_side_effects=True, vmem_limit_bytes=VMEM_GRANT
            ),
        )(*args)
        return pl.pallas_call(
            finish,
            out_shape=(
                jax.ShapeDtypeStruct((rows, cols), f32),
                jax.ShapeDtypeStruct((rows, cols), f32),
                jax.ShapeDtypeStruct((ITERS,), f32),
            ),
            in_specs=[pl.BlockSpec(memory_space=pltpu.VMEM)] * 3,
            out_specs=(
                pl.BlockSpec(memory_space=pl.ANY),
                pl.BlockSpec(memory_space=pl.ANY),
                pl.BlockSpec(memory_space=pl.ANY),
            ),
            scratch_shapes=[
                vmem((rows, cols), f32),
                vmem((rows, cols), f32),
                pltpu.SMEM((ITERS,), f32),
                dma((3,)),
            ],
            compiler_params=pltpu.CompilerParams(vmem_limit_bytes=FINISH_GRANT),
        )(V, U, T)

    return jax.shard_map(
        body,
        mesh=mesh,
        in_specs=(P("lat", "lon"), P(None, "lat", "lon"), P("lat", "lon"), P("lat", "lon")),
        out_specs=(P("lat", "lon"), P("lat", "lon"), P()),
        check_vma=False,
    )
```

```python
import functools

import jax
import jax.numpy as jnp
from jax import lax
from jax.experimental import pallas as pl
from jax.experimental.pallas import tpu as pltpu
from jax.sharding import PartitionSpec as P

DEG = 4
ITERS = 3
LOW_EIG = 0.25
HIGH_EIG = 20.5
LANES = 128
TILE = 8
HALF = 4
STRIP = 16
FIELDS = 7
NGROUPS = 2
ALL_TO_ALL = 64
VMEM_GRANT = 24 * 1024 * 1024
FINISH_GRANT = 4 * 1024 * 1024
MESH = pl.DeviceIdType.MESH


def factored():
    theta = (HIGH_EIG + LOW_EIG) / 2.0
    delta = (HIGH_EIG - LOW_EIG) / 2.0
    sigma = theta / delta
    rho = 1.0 / sigma
    step = at_zero = 1.0 / theta
    for _ in range(DEG - 1):
        rho_new = 1.0 / (2.0 * sigma - rho)
        step = rho_new * rho * step + 2.0 * rho_new / delta
        at_zero = at_zero + step
        rho = rho_new
    bump = theta * theta - delta * delta
    return theta, bump, at_zero / (-2.0 * theta * (theta * theta + bump))


def scalars(h, g):
    ht = [h[k + 1] + h[k] for k in range(len(h) - 1)]

    def form(a, t):
        total = None
        for k in range(2 * len(a) - 1):
            pairs = None
            for i in range(len(a)):
                j = k - i
                if 0 <= j < len(a) and i <= j:
                    term = a[i] * a[j]
                    if i != j:
                        term = term + term
                    pairs = term if pairs is None else pairs + term
            pairs = pairs * t[k]
            total = pairs if total is None else total + pairs
        return total

    one = jnp.ones_like(h[0])
    zero = jnp.zeros_like(h[0])
    a = [one]
    b = [one]
    gamma = h[0]
    norms = [g[0]]
    alpha = gamma / ht[0]
    x = [zero] * ITERS
    beta = zero
    for k in range(ITERS):
        if k > 0:
            b = [a[i] + (beta * b[i] if i < len(b) else 0.0) for i in range(len(a))]
        for i in range(len(b)):
            x[i] = x[i] + alpha * b[i]
        tb = [
            (b[i - 1] if i > 0 else zero) + (b[i] if i < len(b) else zero)
            for i in range(len(b) + 1)
        ]
        a = [(a[i] if i < len(a) else zero) - alpha * tb[i] for i in range(len(tb))]
        if k < ITERS - 1:
            gamma_new = form(a, h)
            dlt = form(a, ht)
            norms.append(form(a, g))
            beta = gamma_new / gamma
            alpha = gamma_new / (dlt - beta * gamma_new / alpha)
            gamma = gamma_new
    return x, a, norms


HPAIRS = [((k + 1) // 2, k // 2) for k in range(2 * ITERS)]
GPAIRS = [(k // 2, (k + 1) // 2) for k in range(2 * ITERS - 1)]
NSUM = len(HPAIRS) + len(GPAIRS)


def cs_of(j):
    return slice(j * LANES, (j + 1) * LANES)


def ts_of(i):
    return slice(i * TILE, (i + 1) * TILE)


def groups_of(nc, count):
    if count == 1:
        return [(0, nc)], [list(range(nc + 1))]
    edges = [-(-nc * g // count) for g in range(count + 1)]
    spans = [(edges[g], edges[g + 1]) for g in range(count)]
    lists = []
    for g, (lo, hi) in enumerate(spans):
        own = list(range(lo, hi))
        own = [nc] + own if g == 0 else [lo - 1] + own
        lists.append(own + [nc] if g == count - 1 else own)
    return spans, lists


def kernel(
    nlat, nlon, rhs_in, coef_in, extra_in, mask_in, V, U, T_out,
    C, E, B, M, SR, RR, SP, RP, CP, K, L2, VC, Z, GS, G, G2,
    LR, loc_sem, snd, rcv, red_s, red_r, rel_s, rel_r, ready,
):
    rows, cols = rhs_in.shape
    nr = rows // TILE
    nc = cols // LANES
    depth = ITERS
    ilat = lax.axis_index("lat")
    ilon = lax.axis_index("lon")
    has_n = ilat < nlat - 1
    has_s = ilat > 0

    local = [
        pltpu.make_async_copy(coef_in, C, loc_sem.at[0]),
        pltpu.make_async_copy(mask_in, M, loc_sem.at[1]),
        pltpu.make_async_copy(extra_in, E, loc_sem.at[2]),
        pltpu.make_async_copy(rhs_in, B, loc_sem.at[3]),
    ]
    for cp in local:
        cp.start()

    def lat_at(d):
        return lax.rem(ilat + d + nlat, nlat)

    def lon_at(d):
        return lax.rem(ilon + d + nlon, nlon)

    def where_to(a, b):
        out = {}
        if a:
            out["lat"] = lat_at(a)
        if b:
            out["lon"] = lon_at(b)
        return out

    barrier = pltpu.get_barrier_semaphore()

    def greet(sem, a, b):
        pl.semaphore_signal(sem, inc=1, device_id=where_to(a, b), device_id_type=MESH)

    for d in range(1, nlat):
        greet(barrier, d, 0)
    for d in range(1, nlon):
        greet(barrier, 0, d)
    for a, there in ((-1, has_s), (1, has_n)):

        @pl.when(there)
        def _():
            greet(barrier, a, -1)
            greet(barrier, a, 1)

    for side, there in ((0, has_n), (1, has_s)):

        @pl.when(jnp.logical_not(there))
        def _():
            RR[side] = jnp.zeros(RR.shape[1:], jnp.float32)
            for e in (0, 1):
                CP[e, side] = jnp.zeros(CP.shape[2:], jnp.float32)

    for cp in local:
        cp.wait()

    def own_field(f, rws, cls):
        if f < 4:
            return C[f, rws, cls]
        if f == 4:
            return E[rws, cls]
        if f == 5:
            return B[rws, cls]
        return M[rws, cls].astype(jnp.float32)

    count = nlat - 1 + nlon - 1 + 2 * (has_n.astype(jnp.int32) + has_s.astype(jnp.int32))
    pl.semaphore_wait(barrier, count)
    direct = nlat * nlon <= ALL_TO_ALL
    if direct:
        for d in range(1, nlon):
            greet(ready, 0, d)

    sub = lax.broadcasted_iota(jnp.int32, (TILE, LANES), 0)
    lane = lax.broadcasted_iota(jnp.int32, (TILE, LANES), 1)
    slot = lane // STRIP
    sends = []
    relays = []
    mid = nlat // 2 - 1
    relaying = nlat % 2 == 0 and nlat >= 4
    at_mid = {1: ilat == mid, -1: ilat == mid + 1}
    at_relay = {1: ilat == nlat - 1, -1: ilat == 0}

    def send(src, dst, a, b, stage):
        i = len(sends)
        cp = pltpu.make_async_remote_copy(
            src_ref=src, dst_ref=dst, send_sem=snd.at[i], recv_sem=rcv.at[i],
            device_id=where_to(a, b), device_id_type=MESH,
        )
        sends.append((cp, a, stage))
        return cp

    def each(cps, a, sending, act):
        def run():
            for cp in cps:
                act(cp)

        if a == 0:
            run()
        elif cps:
            pl.when((has_s if a < 0 else has_n) if sending else (has_n if a < 0 else has_s))(run)

    def start(cps, a):
        each(cps, a, True, lambda cp: cp.start())

    def detour(src, via, dst, a, i):
        k = len(relays)
        ends = {1: (nlat - 1, mid + 1), -1: (0, mid)}[a]
        legs = [
            pltpu.make_async_remote_copy(
                src_ref=src, dst_ref=via, send_sem=snd.at[i], recv_sem=rel_r.at[k],
                device_id={"lat": ends[0]}, device_id_type=MESH,
            ),
            pltpu.make_async_remote_copy(
                src_ref=via, dst_ref=dst, send_sem=rel_s.at[k], recv_sem=rcv.at[i],
                device_id={"lat": ends[1]}, device_id_type=MESH,
            ),
        ]
        relays.append((legs, a))
        return legs

    spans, lists = groups_of(nc, NGROUPS)
    ng = len(spans)
    stage_of = (ng - 1, 0)

    def half_rows(side, k):
        first = k * HALF if side == 0 else rows - (k + 1) * HALF
        return slice(first, first + HALF)

    for g, (lo, hi) in enumerate(spans):
        for side in (0, 1):
            for f in range(FIELDS):
                for k in range(depth):
                    for j in range(lo, hi):
                        SR[side, f * depth + k, :, cs_of(j)] = own_field(f, half_rows(side, k), cs_of(j))
        cl = pl.ds(lo * LANES, (hi - lo) * LANES)
        for a in (-1, 1):
            side = (a + 1) // 2
            move = (SR.at[side, :, :, cl], LR, RR.at[side, :, :, cl])
            i = len(sends)
            cp = send(move[0], move[2], a, 0, g)
            if not (relaying and g == ng - 1):
                start([cp], a)
                continue
            leg = detour(*move, a, i)[0]
            there = has_s if a < 0 else has_n
            pl.when(there & jnp.logical_not(at_mid[a]))(lambda: cp.start())
            pl.when(at_mid[a])(lambda: leg.start())
        if g == 0:
            for side, chunk in ((0, 0), (1, nc - 1)):
                for i in range(nr):
                    strip = jnp.zeros((TILE, LANES), jnp.float32)
                    for f in range(FIELDS):
                        turn = (STRIP * f + side * STRIP) % LANES
                        a = own_field(f, ts_of(i), cs_of(chunk))
                        a = pltpu.roll(a, turn, 1) if turn else a
                        strip = jnp.where(slot == f, a, strip)
                    SP[side, ts_of(i), :] = strip
            start([send(SP.at[e], RP.at[e], 0, 2 * e - 1, stage_of[e]) for e in (1, 0)], 0)
        for e in (0, 1):
            if stage_of[e] != g:
                continue
            for a in (-1, 1):
                src = pl.ds(0, STRIP) if a < 0 else pl.ds(rows - STRIP, STRIP)
                start([send(SP.at[e, src], CP.at[e, (a + 1) // 2], a, 2 * e - 1, g)], a)

    for a in (-1, 1):
        mine = [legs for legs, d in relays if d == a]
        if mine:

            @pl.when(at_relay[a])
            def _():
                for first, second in mine:
                    first.wait_recv()
                    second.start()

    up = sub < HALF
    s0 = sub == 0
    s3 = sub == HALF - 1
    s4 = sub == HALF
    s7 = sub == TILE - 1
    first = lane == 0
    last = lane == LANES - 1
    rims = (lane < STRIP, lane >= LANES - STRIP)

    def roll0(a, n):
        return pltpu.roll(a, n, 0)

    def onion(n8, s8):
        near = jnp.where(up, n8, s8)
        return [near, jnp.where(up, roll0(n8, HALF), roll0(s8, HALF))]

    def raw(f, j, ends):
        if j < nc:
            tiles = [own_field(f, ts_of(i), cs_of(j)) for i in range(nr)]
            for k in range(depth):
                halves = [RR[side, f * depth + k, :, cs_of(j)] for side in (0, 1)]
                tiles.append(jnp.concatenate(halves, axis=0))
            return tiles

        def turned(read):
            out = []
            for e in ends:
                turn = (-STRIP * f - e * STRIP) % LANES
                a = read(e)
                out.append(pltpu.roll(a, turn, 1) if turn else a)
            return jnp.where(lane < LANES // 2, out[0], out[1]) if len(out) > 1 else out[0]

        tiles = [turned(lambda e, i=i: RP[e, ts_of(i), :]) for i in range(nr)]
        n8, n16 = (turned(lambda e, i=i: CP[e, 0, ts_of(i), :]) for i in (0, 1))
        s16, s8 = (turned(lambda e, i=i: CP[e, 1, ts_of(i), :]) for i in (0, 1))
        tiles = tiles + onion(n8, s8) + [jnp.where(up, n16, s16)]
        if f < 6:
            return tiles
        rim = rims[ends[0]] if len(ends) == 1 else rims[0] | rims[1]
        return [jnp.where(rim, t, 0.0) for t in tiles]

    def north(t, n):
        memo = {}

        def r3(i):
            if i not in memo:
                memo[i] = roll0(t[i], HALF - 1)
            return memo[i]

        r7 = [roll0(a, TILE - 1) for a in t]
        out = []
        for i in range(n):
            if i < nr:
                out.append(jnp.where(s7, r7[i + 1], r7[i]))
                continue
            a = jnp.where(s7, r7[0] if i == nr else r3(i - 1), r7[i])
            out.append(jnp.where(s3, r3(i + 1), a) if i + 1 < len(t) else a)
        return out

    def south(t, n):
        memo = {}

        def r5(i):
            if i not in memo:
                memo[i] = roll0(t[i], HALF + 1)
            return memo[i]

        r1 = [roll0(a, 1) for a in t]
        out = []
        for i in range(n):
            if i < nr:
                out.append(jnp.where(s0, r1[i - 1] if i else r1[nr], r1[i]))
                continue
            a = jnp.where(s0, r1[nr - 1] if i == nr else r5(i - 1), r1[i])
            out.append(jnp.where(s4, r5(i + 1), a) if i + 1 < len(t) else a)
        return out

    def shifts(read, order, ring):
        memo = {}

        def get(kind, p):
            p = p % len(order)
            if (kind, p) not in memo:
                if kind == 0:
                    memo[kind, p] = read(order[p])
                else:
                    turn = 1 if kind < 0 else LANES - 1
                    memo[kind, p] = [pltpu.roll(a, turn, 1) for a in get(0, p)]
            return memo[kind, p]

        def east(p):
            if p + 1 == len(order) and not ring:
                return get(1, p)
            return [jnp.where(last, b, a) for a, b in zip(get(1, p), get(1, p + 1))]

        def west(p):
            if p == 0 and not ring:
                return get(-1, p)
            return [jnp.where(first, b, a) for a, b in zip(get(-1, p), get(-1, p - 1))]

        return (lambda p: get(0, p)), east, west

    full = nr + depth
    theta, bump, scale = factored()

    def put(ref, k, j, tiles):
        for i, t in enumerate(tiles):
            ref[k, ts_of(i), cs_of(j)] = t

    def links(order, ring, ends):
        mc, me_of, mw_of = shifts(lambda j: raw(6, j, ends), order, ring)
        for p, j in enumerate(order):
            m, me, mw = mc(p), me_of(p), mw_of(p)
            nm, nme, nmw = north(m, full), north(me, full), north(mw, full)
            for k, f, o in ((1, 0, me), (6, 1, nm)):
                put(K, k, j, [c * a * b for c, a, b in zip(raw(f, j, ends), m, o)])
            for k, f, o in ((0, 2, nme), (1, 3, nmw)):
                put(L2, k, j, [c * a * b for c, a, b in zip(raw(f, j, ends), m, o)])
            for i, (a, b) in enumerate(zip(m, raw(5, j, ends))):
                VC[ts_of(i), cs_of(j)] = a * b

        def tiles_of(ref, k):
            return lambda j: [ref[k, ts_of(i), cs_of(j)] for i in range(full)]

        cle, _, wle_of = shifts(tiles_of(K, 1), order, ring)
        clne, _, wlne_of = shifts(tiles_of(L2, 0), order, ring)
        clnw, elnw_of, _ = shifts(tiles_of(L2, 1), order, ring)
        for p, j in enumerate(order):
            le, wle, lne, wlne = cle(p), wle_of(p), clne(p), wlne_of(p)
            lnw, elnw = clnw(p), elnw_of(p)
            ln = tiles_of(K, 6)(j)
            sln = south(ln, full)
            swlne, selnw = south(wlne, full), south(elnw, full)
            put(K, 2, j, wle)
            put(K, 3, j, sln)
            put(K, 4, j, south(lne, full))
            put(K, 5, j, south(lnw, full))
            put(K, 7, j, wlne)
            put(K, 8, j, elnw)
            for i, d in enumerate(raw(4, j, ends)):
                d = d + le[i] + wle[i] + ln[i] + sln[i]
                d = d + lne[i] + swlne[i] + lnw[i] + selnw[i]
                K[0, ts_of(i), cs_of(j)] = d
                K[9, ts_of(i), cs_of(j)] = d - theta
                K[10, ts_of(i), cs_of(j)] = d - 2.0 * theta

    def apply(order, ring, ref, diag, n_in, n_out, finish, skip=()):
        centre, east, west = shifts(
            lambda j: [ref[ts_of(i), cs_of(j)] for i in range(n_in)], order, ring
        )
        used = min(n_in, n_out + 1)
        for p, j in enumerate(order):
            if j in skip:
                continue
            v, ve, vw = centre(p), east(p), west(p)

            def k(n, i):
                return K[n, ts_of(i), cs_of(j)]

            up_part = [k(3, i) * v[i] + k(4, i) * ve[i] + k(5, i) * vw[i] for i in range(used)]
            low_part = [k(6, i) * v[i] + k(7, i) * vw[i] + k(8, i) * ve[i] for i in range(used)]
            np_ = north(up_part, n_out)
            sq = south(low_part, n_out)
            for i in range(n_out):
                a = k(diag, i) * v[i] - k(1, i) * ve[i] - k(2, i) * vw[i] - np_[i] - sq[i]
                finish(i, j, a)

    seen = set()

    def record(ref, n, i, j, value):
        if i >= nr or j == nc:
            return
        if j in seen:
            value = jnp.where(lane < LANES // 2, ref[n, ts_of(i), cs_of(j)], value)
        ref[n, ts_of(i), cs_of(j)] = value

    def rounds(order, ring):
        for j in order:
            for i in range(nr):
                record(V, 0, i, j, VC[ts_of(i), cs_of(j)])
        for it in range(ITERS):
            n = full - it

            def level0(i, j, a):
                Z[0, ts_of(i), cs_of(j)] = a

            def level1(i, j, a):
                at = (ts_of(i), cs_of(j))
                Z[1, ts_of(i), cs_of(j)] = scale * a + (scale * bump) * VC[at]

            def level2(i, j, a):
                Z[0, ts_of(i), cs_of(j)] = a
                record(U, it, i, j, a)

            def last_level(i, j, a):
                at = (ts_of(i), cs_of(j))
                new = a - VC[at]
                if it < ITERS - 1:
                    VC[at] = new
                record(V, it + 1, i, j, new)

            apply(order, ring, VC, 9, n, n, level0)
            apply(order, ring, Z.at[0], 9, n, n, level1)
            apply(order, ring, Z.at[1], 10, n, n, level2)
            skip = (nc,) if it == ITERS - 1 else ()
            apply(order, ring, Z.at[0], 0, n, n - 1, last_level, skip)

    acc = [None] * NSUM
    waited = 0
    for g, order in enumerate(lists):
        for a in (0, -1, 1):
            cps = [cp for cp, d, stage in sends if d == a and stage == g]
            each(cps, a, False, lambda cp: cp.wait_recv())
        ring = len(lists) == 1
        links(order, ring, [e for e in (0, 1) if stage_of[e] == g])
        rounds(order, ring)
        done = [j for j in order if j < nc and (ring or g == len(lists) - 1 or j != order[-1])]
        for j in done:
            for i in range(nr):
                v = [V[n, ts_of(i), cs_of(j)] for n in range(ITERS + 1)]
                u = [U[n, ts_of(i), cs_of(j)] for n in range(ITERS)]
                new = [v[a] * u[b] for a, b in HPAIRS] + [v[a] * v[b] for a, b in GPAIRS]
                acc = [b if a is None else a + b for a, b in zip(acc, new)]
        seen.update(j for j in order if j < nc)

    row = jnp.zeros((TILE, LANES), jnp.float32)
    for n, a in enumerate(acc):
        row = jnp.where(lane == n, jnp.sum(a, axis=1, keepdims=True), row)
    row = jnp.sum(row, axis=0, keepdims=True)

    pending = []
    paired = nlat & (nlat - 1) == 0

    def peer(a, b):
        if not paired:
            return where_to(a, b)
        to, bit = ilat, 1
        while bit < nlat:
            if a & bit:
                to = to + bit - 2 * bit * (lax.div(ilat, bit) % 2)
            bit *= 2
        return {"lat": to, "lon": lon_at(b)}

    def drain():
        for a in (0, -1, 1):
            cps = [cp for cp, d, _ in sends if d == a]
            each(cps, a, True, lambda cp: cp.wait_send())
        for a in (-1, 1):
            mine = [legs for legs, d in relays if d == a]
            if mine:

                @pl.when(at_relay[a])
                def _():
                    for _, second in mine:
                        second.wait_send()

    def gather(row, stage, buf, me, peers):
        GS[stage] = row
        buf[me] = row
        cps = []
        for a, b in peers:
            i = len(pending)
            cp = pltpu.make_async_remote_copy(
                src_ref=GS.at[stage], dst_ref=buf.at[me],
                send_sem=red_s.at[i], recv_sem=red_r.at[i],
                device_id=peer(a, b), device_id_type=MESH,
            )
            cp.start()
            cps.append(cp)
            pending.append(cp)
        if stage == 0:
            drain()
        for cp in cps:
            cp.wait_send()
        for cp in cps[::-1]:
            cp.wait_recv()
        parts = [buf[n] for n in range(buf.shape[0])]
        while len(parts) > 1:
            odd = parts[len(parts) // 2 * 2 :]
            parts = [a + b for a, b in zip(parts[::2], parts[1::2])] + odd
        return parts[0]

    if direct:
        pl.semaphore_wait(ready, nlon - 1)
        peers = [(a, b) for a in range(nlat) for b in range(nlon) if a or b][::-1]
        row = gather(row, 0, G, ilat * nlon + ilon, peers)
    else:
        row = gather(row, 0, G, ilat, [(d, 0) for d in range(1, nlat)])
        row = gather(row, 1, G2, ilon, [(0, d) for d in range(1, nlon)])
    T_out[...] = jnp.broadcast_to(row, (TILE, LANES))


def finish(V, U, T, x_out, r_out, n_out, X, R, N, sems):
    rows, cols = X.shape
    total = T[...]
    sums = [jnp.broadcast_to(total[:, n : n + 1], (TILE, LANES)) for n in range(NSUM)]
    xs, rs, norms = scalars(sums[: len(HPAIRS)], sums[len(HPAIRS) :])
    for n in range(ITERS):
        N[n] = norms[n][0, 0]
    cps = [pltpu.make_async_copy(N, n_out, sems.at[0])]
    cps[0].start()
    for buf, out, co, src in ((X, x_out, xs, U), (R, r_out, rs, V)):
        for j in range(cols // LANES):
            for i in range(rows // TILE):
                at = (ts_of(i), cs_of(j))
                a = co[0] * src[0, ts_of(i), cs_of(j)]
                for n in range(1, len(co)):
                    a = a + co[n] * src[n, ts_of(i), cs_of(j)]
                buf[at] = a
        cp = pltpu.make_async_copy(buf, out, sems.at[len(cps)])
        cp.start()
        cps.append(cp)
    for cp in cps:
        cp.wait()


def solution(mesh):
    nlat = mesh.shape["lat"]
    nlon = mesh.shape["lon"]

    def body(*args):
        rows, cols = args[0].shape
        nc = cols // LANES
        W = cols + LANES
        R = rows + ITERS * TILE
        f32, i32 = jnp.float32, jnp.int32
        ndev = nlat * nlon
        direct = ndev <= ALL_TO_ALL
        npeers = ndev - 1 if direct else nlat + nlon - 2
        nsend = 6 + 2 * NGROUPS
        lo, hi = groups_of(nc, NGROUPS)[0][-1]
        half = (hi - lo) * LANES
        vmem, dma = pltpu.VMEM, pltpu.SemaphoreType.DMA
        args = [pltpu.with_memory_space_constraint(a, pltpu.HBM) for a in args]
        V, U, T = pl.pallas_call(
            functools.partial(kernel, nlat, nlon),
            out_shape=(
                vmem((ITERS + 1, rows, cols), f32),
                vmem((ITERS, rows, cols), f32),
                vmem((TILE, LANES), f32),
            ),
            in_specs=[pl.BlockSpec(memory_space=pl.ANY)] * 4,
            out_specs=(pl.BlockSpec(memory_space=pltpu.VMEM),) * 3,
            scratch_shapes=[
                vmem((4, rows, cols), f32),
                vmem((rows, cols), f32),
                vmem((rows, cols), f32),
                vmem((rows, cols), i32),
                vmem((2, FIELDS * ITERS, HALF, cols), f32),
                vmem((2, FIELDS * ITERS, HALF, cols), f32),
                vmem((2, rows, LANES), f32),
                vmem((2, rows, LANES), f32),
                vmem((2, 2, STRIP, LANES), f32),
                vmem((11, R, W), f32),
                vmem((2, R, W), f32),
                vmem((R, W), f32),
                vmem((2, R, W), f32),
                vmem((2, 1, LANES), f32),
                vmem((ndev if direct else nlat, 1, LANES), f32),
                vmem((nlon, 1, LANES), f32),
                vmem((FIELDS * ITERS, HALF, half), f32),
                dma((4,)),
                dma((nsend,)),
                dma((nsend,)),
                dma((npeers,)),
                dma((npeers,)),
                dma((2,)),
                dma((2,)),
                pltpu.SemaphoreType.REGULAR,
            ],
            compiler_params=pltpu.CompilerParams(
                collective_id=0, has_side_effects=True, vmem_limit_bytes=VMEM_GRANT
            ),
        )(*args)
        return pl.pallas_call(
            finish,
            out_shape=(
                jax.ShapeDtypeStruct((rows, cols), f32),
                jax.ShapeDtypeStruct((rows, cols), f32),
                jax.ShapeDtypeStruct((ITERS,), f32),
            ),
            in_specs=[pl.BlockSpec(memory_space=pltpu.VMEM)] * 3,
            out_specs=(
                pl.BlockSpec(memory_space=pl.ANY),
                pl.BlockSpec(memory_space=pl.ANY),
                pl.BlockSpec(memory_space=pl.ANY),
            ),
            scratch_shapes=[
                vmem((rows, cols), f32),
                vmem((rows, cols), f32),
                pltpu.SMEM((ITERS,), f32),
                dma((3,)),
            ],
            compiler_params=pltpu.CompilerParams(vmem_limit_bytes=FINISH_GRANT),
        )(V, U, T)

    return jax.shard_map(
        body,
        mesh=mesh,
        in_specs=(P("lat", "lon"), P(None, "lat", "lon"), P("lat", "lon"), P("lat", "lon")),
        out_specs=(P("lat", "lon"), P("lat", "lon"), P()),
        check_vma=False,
    )
```
